128 devices in a mesh: section: 4 (over x), expert: 32 (over z, y, core).
Axes of the slice: x: 4, y: 4, z: 4, core: 2. Of those that a mesh axis runs over, the one named last changes fastest.
Arguments:
- section_inputs: float32 [4, 4096, 2048], P('section', 'expert'), may hold values from -6 to 6
- stored_inputs: float32 [4, 4096, 2048], P('section', 'expert'), may hold values from -6 to 6
- out_grads: bfloat16 [4, 4096, 2048], P('section', 'expert'), may hold values from -6 to 6
- fwd_routes: int32 [4, 4096, 2], P('section', 'expert'), may hold values from 0 to 15, all different within a row; in each aligned block of 128 rows (0 to 127, 128 to 255, ..., all dimensions but the last counted through in order) at most 20 rows name the same one
- fwd_gates: float32 [4, 4096, 2], P('section', 'expert'), may hold values from 0.2 to 1
- fwd_modulation: float32 [4, 3, 2048], P('section'), may hold values from -3 to 3
- bwd_routes: int32 [4, 4096, 2], P('section', 'expert'), may hold values from 0 to 15, all different within a row; in each aligned block of 128 rows (0 to 127, 128 to 255, ..., all dimensions but the last counted through in order) at most 20 rows name the same one
- bwd_gates: float32 [4, 4096, 2], P('section', 'expert'), may hold values from 0.2 to 1
- bwd_modulation: float32 [4, 3, 2048], P('section'), may hold values from -3 to 3
- up_weight: bfloat16 [4, 32, 2048, 1024], P('section', 'expert'), may hold values from -0.125 to 0.125
- down_weight: bfloat16 [4, 32, 1024, 2048], P('section', 'expert'), may hold values from -0.125 to 0.125
Outputs:
- next_inputs: float32 [4, 4096, 2048], P('section', 'expert')
- input_grads: bfloat16 [4, 4096, 2048], P('section', 'expert')
The draws below stay inside these ranges and needn't reach their ends.
Inputs may be any that keep to these rules, and one draw needn't show every extreme that they name: `fwd_routes`: A token names two different experts. In the rows of one index of expert (aligned blocks of 128 rows of a section) no expert is named more than 20 times, a bound that some block reaches. `bwd_routes`: A token names two different experts. In the rows of one index of expert (aligned blocks of 128 rows of a section) no expert is named more than 20 times, a bound that some block reaches.
All inputs are finite; a program needn't handle non-finite values.
Results may differ from the reference program's by a relative error of at most 0.0042.
Values may be sent and summed in bfloat16 or wider, within the bound.
No kernel may reach another device: no remote copies, remote signals or barrier semaphores. Data moves between devices by JAX's collectives and lax.ppermute only.
A program may use at most 128 MiB of HBM per device.

```python
import math
import jax
import jax.numpy as jnp
import numpy as np
from jax import lax

D = 2048
FF = 2048
FF_DEV = 1024
TOK_DEV = 128
TOKENS = 4096
EXPERTS = 16
CAP = 20
N_SECTION = 4
N_EXPERT = 32


def levels(rng, dims, split, smallest, top_value):
    def one(position, shards_of):
        draws = jax.random.uniform(jax.random.fold_in(jax.random.fold_in(rng, 6), position), (shards_of,), jnp.float32, smallest / len(split), top_value / len(split))
        return jnp.repeat(jnp.exp(draws), dims[position] // shards_of).reshape((-1,) + (1,) * (len(dims) - position - 1))

    gain = one(*split[0])
    for cut in split[1:]:
        gain = gain * one(*cut)
    return gain


def routed_block(key, own, number, rows, number_of, top, limit, lean):
    ranking = jax.random.permutation(key, number_of)
    crowded, ordinary = load_shares(number_of, rows * top, limit, lean, True), load_shares(number_of, rows * top, limit, lean, False)
    places = jnp.arange(number_of)

    def named(tallies, turn):
        used = int((tallies > 0).sum())
        fixed = max(1, used // 4)
        passed = fixed + (places - fixed + turn * (used - fixed)) % max(1, number_of - fixed)
        return jnp.zeros((number_of,), jnp.int32).at[ranking[jnp.where(places < fixed, places, passed)]].set(jnp.asarray(tallies, jnp.int32))

    tallies = jnp.where(number % 4 == 0, named(crowded, number // 4), named(ordinary, number - number // 4 - 1))
    mixed = jax.random.permutation(jax.random.fold_in(own, 3), number_of)
    giver, receiver = mixed[0:number_of // 2 * 2:2], mixed[1:number_of // 2 * 2:2]
    slack = jnp.minimum(tallies[giver] - 1, limit - tallies[receiver]) // 2
    slack = jnp.where((giver == ranking[0]) | (receiver == ranking[0]) | (tallies[receiver] == 0), 0, jnp.maximum(slack, 0))
    passed = jax.random.randint(jax.random.fold_in(own, 4), (number_of // 2,), 0, 1 << 20) % (slack + 1)
    tallies = tallies.at[giver].add(-passed).at[receiver].add(passed)
    items = jnp.searchsorted(jnp.cumsum(tallies), jnp.arange(rows * top), side="right").astype(jnp.int32)
    table = items.reshape(top, rows).T
    table = table[jax.random.permutation(jax.random.fold_in(own, 1), rows)]
    turn = jax.random.randint(jax.random.fold_in(own, 2), (rows, 1), 0, top)
    return jnp.take_along_axis(table, (jnp.arange(top)[None, :] + turn) % top, axis=1)


def load_shares(count, total, most, slope, full):
    weights = [(1 << 20) // math.isqrt(standing ** slope) + 1 for standing in range(1, count + 1)]
    largest = most if full else min(most, max(-(-total // count), total * weights[0] // sum(weights)))
    least = 1 if total - largest >= count - 1 else 0
    counts, rest = [largest] + [least] * (count - 1), total - largest - least * (count - 1)
    while rest > 0:
        movable = [i for i in range(1, count) if counts[i] < largest] or [i for i in range(1, count) if counts[i] < most]
        whole, remaining = sum([weights[i] for i in movable]), rest
        for i in movable:
            more = min(most - counts[i], max(1, remaining * weights[i] // whole), rest)
            counts[i] = counts[i] + more
            rest = rest - more
    return np.array(counts)


def normal_values(stream_key, dims, width, most, split=(), held_as=jnp.bfloat16):
    drawn = width * jax.random.normal(stream_key, dims, jnp.float32)
    if split:
        drawn = drawn * levels(stream_key, dims, split, -0.22, 0.18)
    return jnp.clip(drawn, -most, most).astype(held_as)


def setup_inputs(seed: int = 0) -> dict:
    keys = jax.random.split(jax.random.key(seed), 12)
    section_inputs = normal_values(keys[0], (N_SECTION, TOKENS, D), 1.0, 6.0, ((0, 4), (1, 32)), jnp.float32)
    stored_inputs = normal_values(keys[1], (N_SECTION, TOKENS, D), 1.0, 6.0, ((0, 4), (1, 32)), jnp.float32)
    out_grads = normal_values(keys[2], (N_SECTION, TOKENS, D), 1.0, 6.0, ((0, 4), (1, 32)))
    fwd_routes_keys = jax.random.split(jax.random.fold_in(keys[3], 1), N_SECTION * TOKENS // TOK_DEV)
    fwd_routes_turns = jax.random.permutation(jax.random.fold_in(keys[3], 3), N_SECTION * TOKENS // TOK_DEV)
    fwd_routes = jax.vmap(lambda own, number: routed_block(jax.random.fold_in(keys[3], 2), own, number, TOK_DEV, EXPERTS, 2, CAP, 2))(fwd_routes_keys, fwd_routes_turns).reshape((N_SECTION, TOKENS, 2))
    fwd_gates = jnp.clip(0.2 + 0.8 * jax.random.uniform(keys[4], (N_SECTION, TOKENS, 2), jnp.float32) ** levels(keys[4], (N_SECTION, TOKENS, 2), ((0, 4), (1, 32)), -0.2, 0.2), 0.2, 1.0)
    fwd_modulation = normal_values(keys[5], (N_SECTION, 3, D), 0.5, 3.0, ((0, 4),), jnp.float32)
    bwd_routes_keys = jax.random.split(jax.random.fold_in(keys[6], 1), N_SECTION * TOKENS // TOK_DEV)
    bwd_routes_turns = jax.random.permutation(jax.random.fold_in(keys[6], 3), N_SECTION * TOKENS // TOK_DEV)
    bwd_routes = jax.vmap(lambda own, number: routed_block(jax.random.fold_in(keys[6], 2), own, number, TOK_DEV, EXPERTS, 2, CAP, 2))(bwd_routes_keys, bwd_routes_turns).reshape((N_SECTION, TOKENS, 2))
    bwd_gates = jnp.clip(0.2 + 0.8 * jax.random.uniform(keys[7], (N_SECTION, TOKENS, 2), jnp.float32) ** levels(keys[7], (N_SECTION, TOKENS, 2), ((0, 4), (1, 32)), -0.2, 0.2), 0.2, 1.0)
    bwd_modulation = normal_values(keys[8], (N_SECTION, 3, D), 0.5, 3.0, ((0, 4),), jnp.float32)
    up_weight = normal_values(keys[9], (N_SECTION, N_EXPERT, D, FF_DEV), D ** -0.5, 0.125, ((0, 4), (1, 32)))
    down_weight = normal_values(keys[10], (N_SECTION, N_EXPERT, FF_DEV, D), FF ** -0.5, 0.125, ((0, 4), (1, 32)))
    return dict(section_inputs=section_inputs, stored_inputs=stored_inputs, out_grads=out_grads, fwd_routes=fwd_routes, fwd_gates=fwd_gates, fwd_modulation=fwd_modulation, bwd_routes=bwd_routes, bwd_gates=bwd_gates, bwd_modulation=bwd_modulation, up_weight=up_weight, down_weight=down_weight)


norm_eps = 1e-06

def layer_norm(tok_rows):
    mean_row = lax.optimization_barrier(jnp.mean(tok_rows, axis=-1, keepdims=True))
    centered = tok_rows - mean_row
    variance = lax.optimization_barrier(jnp.mean(centered * centered, axis=-1, keepdims=True))
    inv_std = lax.rsqrt(variance + norm_eps)
    return (centered * inv_std, inv_std)

def slot_numbers(routes):
    flat_ids = routes.reshape(-1).astype(jnp.int32)
    choose = (flat_ids[:, None] == jnp.arange(EXPERTS, dtype=jnp.int32)[None, :]).astype(jnp.int32)
    before = jnp.cumsum(choose, axis=0) - choose
    return (flat_ids, lax.optimization_barrier(jnp.sum(before * choose, axis=1)).astype(jnp.int32))

def place_rows(flat_ids, slot_index, pair_values):
    empty = jnp.zeros((EXPERTS, N_EXPERT * CAP, D), pair_values.dtype)
    return empty.at[flat_ids, slot_index].set(pair_values)

def one_section(packed):
    inputs, stored, grads, fwd_routes, fwd_gates, fwd_mod, bwd_routes, bwd_gates, bwd_mod, up_w, down_w = packed
    up_all = up_w.reshape(EXPERTS, 2, D, FF_DEV).astype(jnp.float32)
    down_all = down_w.reshape(EXPERTS, 2, FF_DEV, D).astype(jnp.float32)
    normed, _ = layer_norm(inputs)
    hidden = (normed * (1.0 + fwd_mod[1]) + fwd_mod[0]).astype(jnp.bfloat16)
    flat_ids, slot_index = slot_numbers(fwd_routes)
    rows = place_rows(flat_ids, slot_index, jnp.repeat(hidden, 2, axis=0)).astype(jnp.float32)
    pre_act = jnp.einsum('erd,ejdf->ejrf', rows, up_all)
    activation = jax.nn.gelu(pre_act).astype(jnp.bfloat16).astype(jnp.float32)
    partial_value = jnp.einsum('ejrf,ejfd->ejrd', activation, down_all).astype(jnp.bfloat16).astype(jnp.float32)
    summed = partial_value[:, 0] + partial_value[:, 1]
    pair_out = summed[flat_ids, slot_index].reshape(TOKENS, 2, D)
    moe_out = lax.optimization_barrier(jnp.sum(pair_out * fwd_gates[:, :, None], axis=1))
    out_fwd = inputs + fwd_mod[2] * moe_out
    normed_b, inv_b = layer_norm(stored)
    hidden_b = (normed_b * (1.0 + bwd_mod[1]) + bwd_mod[0]).astype(jnp.bfloat16)
    grad_rows = grads.astype(jnp.float32)
    pair_grads = (bwd_gates[:, :, None] * (bwd_mod[2] * grad_rows)[:, None, :]).astype(jnp.bfloat16).reshape(2 * TOKENS, D)
    flat_b, slot_b = slot_numbers(bwd_routes)
    rows_h = place_rows(flat_b, slot_b, jnp.repeat(hidden_b, 2, axis=0)).astype(jnp.float32)
    rows_g = place_rows(flat_b, slot_b, pair_grads).astype(jnp.float32)
    pre_b = jnp.einsum('erd,ejdf->ejrf', rows_h, up_all)
    act_grad = jnp.einsum('erd,ejfd->ejrf', rows_g, down_all)
    pre_grad = jax.vjp(jax.nn.gelu, pre_b)[1](act_grad)[0].astype(jnp.bfloat16).astype(jnp.float32)
    part_b = jnp.einsum('ejrf,ejdf->ejrd', pre_grad, up_all).astype(jnp.bfloat16).astype(jnp.float32)
    summed_b = part_b[:, 0] + part_b[:, 1]
    dhidden = lax.optimization_barrier(jnp.sum(summed_b[flat_b, slot_b].reshape(TOKENS, 2, D), axis=1))
    dnorm = dhidden * (1.0 + bwd_mod[1])
    mean_one = lax.optimization_barrier(jnp.mean(dnorm, axis=-1, keepdims=True))
    mean_two = lax.optimization_barrier(jnp.mean(dnorm * normed_b, axis=-1, keepdims=True))
    section_grad = (grad_rows + (dnorm - mean_one - normed_b * mean_two) * inv_b).astype(jnp.bfloat16)
    return (out_fwd, section_grad)

def reference(section_inputs, stored_inputs, out_grads, fwd_routes, fwd_gates, fwd_modulation, bwd_routes, bwd_gates, bwd_modulation, up_weight, down_weight):
    out_fwd, section_grad = lax.map(one_section, (section_inputs, stored_inputs, out_grads, fwd_routes, fwd_gates, fwd_modulation, bwd_routes, bwd_gates, bwd_modulation, up_weight, down_weight))
    next_inputs = jnp.concatenate([jnp.zeros_like(out_fwd[:1]), out_fwd[:-1]], axis=0)
    input_grads = jnp.concatenate([section_grad[1:], jnp.zeros_like(section_grad[:1])], axis=0)
    return (next_inputs, input_grads)
```

```python
import functools

import jax
import jax.numpy as jnp
from jax import lax
from jax.experimental import pallas as pl
from jax.experimental.pallas import tpu as pltpu
from jax.sharding import PartitionSpec as P

norm_eps = 1e-06
f32 = jnp.float32
bf16 = jnp.bfloat16
SPLIT = 2
GROUP = 4


def dot(a, b, dims=((1,), (0,))):
    return lax.dot_general(a, b, (dims, ((), ())), preferred_element_type=f32)


def iota(shape, dim):
    return lax.broadcasted_iota(jnp.int32, shape, dim)


def ones_where(cond):
    return jnp.where(cond, 1.0, 0.0)


def layer_norm(rows):
    mean_row = jnp.mean(rows, axis=-1, keepdims=True)
    centered = rows - mean_row
    variance = jnp.mean(centered * centered, axis=-1, keepdims=True)
    inv_std = lax.rsqrt(variance + norm_eps)
    return centered * inv_std, inv_std


def slot_rows(routes, experts, per_expert):
    tokens = routes.shape[1]
    earlier = ones_where(iota((tokens, tokens), 0) < iota((tokens, tokens), 1)).astype(bf16)
    numbers = iota((experts, tokens), 0)
    chosen = [ones_where(numbers == routes[k : k + 1, :]) for k in range(2)]
    before = [dot(c.astype(bf16), earlier) for c in chosen]
    before[1] = before[1] + jnp.sum(chosen[0], axis=1, keepdims=True)
    slots = [jnp.sum(b * c, axis=0, keepdims=True) for b, c in zip(before, chosen)]
    return [routes[k : k + 1, :] * per_expert + slots[k].astype(jnp.int32) for k in range(2)]


def pack_fwd_body(x_ref, mod_ref, route_ref, out_ref, *, experts, cap):
    normed, _ = layer_norm(x_ref[...])
    hidden = (normed * (1.0 + mod_ref[1]) + mod_ref[0]).astype(bf16)
    part = hidden.shape[1] // SPLIT
    first = slot_rows(route_ref[...], experts, SPLIT * cap)
    numbers = iota((out_ref.shape[0], hidden.shape[0]), 0)
    left, right = [], []
    for h in range(SPLIT):
        hit = (numbers == first[0] + h * cap) | (numbers == first[1] + h * cap)
        left.append(ones_where(hit).astype(bf16))
        right.append(hidden[:, h * part : (h + 1) * part])
    out_ref[...] = dot(jnp.concatenate(left, 1), jnp.concatenate(right, 0)).astype(bf16)


def pack_bwd_body(x_ref, g_ref, gate_ref, mod_ref, route_ref, out_ref, norm_ref, inv_ref, *, experts, cap):
    normed, inv = layer_norm(x_ref[...])
    norm_ref[...] = normed
    inv_ref[...] = inv
    hidden = (normed * (1.0 + mod_ref[1]) + mod_ref[0]).astype(bf16)
    tokens, width = hidden.shape
    part = width // SPLIT
    scaled = mod_ref[2] * g_ref[...].astype(f32)
    gates = jnp.transpose(jnp.concatenate([gate_ref[...]] * 4, 0))
    pair = [(gates[:, k : k + 1] * scaled).astype(bf16) for k in range(2)]
    first = slot_rows(route_ref[...], experts, 2 * SPLIT * cap)
    numbers = iota((out_ref.shape[0], tokens), 0)
    left, right = [], []
    for h in range(SPLIT):
        hit = (numbers == first[0] + h * cap) | (numbers == first[1] + h * cap)
        left.append(ones_where(hit).astype(bf16))
        right.append(hidden[:, h * part : (h + 1) * part])
        for k in range(2):
            left.append(ones_where(numbers == first[k] + (SPLIT + h) * cap).astype(bf16))
            right.append(pair[k][:, h * part : (h + 1) * part])
    out_ref[...] = dot(jnp.concatenate(left, 1), jnp.concatenate(right, 0)).astype(bf16)


def regroup_matrix(kinds, cap, forward):
    size = GROUP * kinds * cap
    by_kind, by_source = iota((size, size), 0 if forward else 1), iota((size, size), 1 if forward else 0)

    def block_of(r):
        return jnp.floor((r.astype(f32) + 0.5) * (1.0 / cap)).astype(jnp.int32)

    kb, sb = block_of(by_kind), block_of(by_source)
    shift = kinds.bit_length() - 1
    same_slot = (by_kind - kb * cap) == (by_source - sb * cap)
    return ones_where(same_slot & (kb == (sb & (kinds - 1)) * GROUP + (sb >> shift))).astype(bf16)


def unpack(x_ref, targets, cap):
    kinds = len(targets) * SPLIT
    matrix = regroup_matrix(kinds, cap, True)
    size, slab, part = GROUP * kinds * cap, GROUP * cap, x_ref.shape[1]
    for n in range(x_ref.shape[0] // size):
        rows = dot(matrix, x_ref[n * size : (n + 1) * size, :]).astype(bf16)
        for t, target in enumerate(targets):
            for h in range(SPLIT):
                kind = t * SPLIT + h
                target[n * slab : (n + 1) * slab, h * part : (h + 1) * part] = rows[kind * slab : (kind + 1) * slab, :]


def repack(acc_ref, out_ref, cap):
    matrix = regroup_matrix(SPLIT, cap, False)
    size, slab, part = GROUP * SPLIT * cap, GROUP * cap, out_ref.shape[1]
    for n in range(out_ref.shape[0] // size):
        rows = [acc_ref[n * slab : (n + 1) * slab, h * part : (h + 1) * part].astype(bf16) for h in range(SPLIT)]
        out_ref[n * size : (n + 1) * size, :] = dot(matrix, jnp.concatenate(rows, 0)).astype(bf16)


def add_to(acc_ref, value, first):
    @pl.when(first)
    def _():
        acc_ref[...] = value

    @pl.when(jnp.logical_not(first))
    def _():
        acc_ref[...] += value


def expert_fwd_body(x_ref, up_a, down_a, up_b, down_b, out_ref, rows_ref, acc_ref, *, cap, blocks):
    step = pl.program_id(0)

    @pl.when(step == 0)
    def _():
        unpack(x_ref, [rows_ref], cap)

    def one(up_ref, down_ref):
        act = jax.nn.gelu(dot(rows_ref[...], up_ref[...])).astype(bf16)
        add_to(acc_ref, dot(act, down_ref[...]), step == 0)

    pl.when(step < blocks)(lambda: one(up_a, down_a))
    pl.when(step >= blocks)(lambda: one(up_b, down_b))

    @pl.when(step == 2 * blocks - 1)
    def _():
        repack(acc_ref, out_ref, cap)


def gelu_slope(x):
    c = 0.7978845608028654
    square = x * x
    t = jnp.tanh(c * x * (1.0 + 0.044715 * square))
    return 0.5 * (1.0 + t) + (0.5 * c) * x * (1.0 - t * t) * (1.0 + (3.0 * 0.044715) * square)


def expert_bwd_body(x_ref, up_a, down_a, up_b, down_b, out_ref, rows_ref, grads_ref, acc_ref, *, cap, blocks):
    step = pl.program_id(0)

    @pl.when(step == 0)
    def _():
        unpack(x_ref, [rows_ref, grads_ref], cap)

    def one(up_ref, down_ref):
        up = up_ref[...]
        slope = gelu_slope(dot(rows_ref[...], up))
        act_grad = dot(grads_ref[...], down_ref[...], ((1,), (1,)))
        add_to(acc_ref, dot((act_grad * slope).astype(bf16), up, ((1,), (1,))), step == 0)

    pl.when(step < blocks)(lambda: one(up_a, down_a))
    pl.when(step >= blocks)(lambda: one(up_b, down_b))

    @pl.when(step == 2 * blocks - 1)
    def _():
        repack(acc_ref, out_ref, cap)


def combine_fwd_body(r_ref, gate_ref, route_ref, x_ref, mod_ref, out_ref, *, experts, cap):
    tokens, width = x_ref.shape
    part = width // SPLIT
    first = slot_rows(route_ref[...], experts, SPLIT * cap)
    numbers = iota((r_ref.shape[0], tokens), 0)
    for h in range(SPLIT):
        weights = sum(jnp.where(numbers == first[k] + h * cap, gate_ref[k : k + 1, :], 0.0) for k in range(2))
        high = weights.astype(bf16)
        low = (weights - high.astype(f32)).astype(bf16)
        both = dot(high, r_ref[...], ((0,), (0,))) + dot(low, r_ref[...], ((0,), (0,)))
        cols = slice(h * part, (h + 1) * part)
        out_ref[:, cols] = x_ref[:, cols] + mod_ref[2][:, cols] * both


def combine_bwd_body(r_ref, route_ref, norm_ref, inv_ref, g_ref, mod_ref, out_ref, *, experts, cap):
    tokens = norm_ref.shape[0]
    first = slot_rows(route_ref[...], experts, SPLIT * cap)
    numbers = iota((r_ref.shape[0], tokens), 0)
    halves = []
    for h in range(SPLIT):
        hit = (numbers == first[0] + h * cap) | (numbers == first[1] + h * cap)
        halves.append(dot(ones_where(hit).astype(bf16), r_ref[...], ((0,), (0,))))
    normed = norm_ref[...]
    dnorm = jnp.concatenate(halves, 1) * (1.0 + mod_ref[1])
    mean_one = jnp.mean(dnorm, axis=-1, keepdims=True)
    mean_two = jnp.mean(dnorm * normed, axis=-1, keepdims=True)
    grad = g_ref[...].astype(f32) + (dnorm - mean_one - normed * mean_two) * inv_ref[...]
    out_ref[...] = grad.astype(bf16)


def call(body, outs, args, flops, **statics):
    moved = sum(a.size * a.dtype.itemsize for a in list(args) + list(outs))
    return pl.pallas_call(
        functools.partial(body, **statics),
        out_shape=outs,
        cost_estimate=pl.CostEstimate(flops=flops, bytes_accessed=moved, transcendentals=0),
    )(*args)


def call_expert(body, rows, weights, scratch_rows, flops, cap, block=512):
    up, down = weights[0]
    width, ff = up.shape
    blocks = ff // block
    slots = rows.shape[0] * rows.shape[1] // width // scratch_rows
    own = lambda i: jnp.minimum(i, blocks - 1)
    other = lambda i: jnp.maximum(i - blocks, 0)
    whole = lambda shape: pl.BlockSpec(shape, lambda i: (0, 0))
    out = jax.ShapeDtypeStruct((slots * SPLIT, width // SPLIT), bf16)
    specs = [whole(rows.shape)]
    for pick in (own, other):
        specs.append(pl.BlockSpec((width, block), lambda i, pick=pick: (0, pick(i))))
        specs.append(pl.BlockSpec((block, width), lambda i, pick=pick: (pick(i), 0)))
    moved = 2 * (rows.size + out.size + 2 * up.size + 2 * down.size)
    return pl.pallas_call(
        functools.partial(body, cap=cap, blocks=blocks),
        out_shape=out,
        grid=(2 * blocks,),
        in_specs=specs,
        out_specs=whole(out.shape),
        scratch_shapes=[pltpu.VMEM((slots, width), bf16)] * scratch_rows + [pltpu.VMEM((slots, width), f32)],
        cost_estimate=pl.CostEstimate(flops=flops, bytes_accessed=moved, transcendentals=0),
        compiler_params=pltpu.CompilerParams(dimension_semantics=("arbitrary",)),
    )(rows, up, down, *weights[1])


def shifted(value, axis, steps):
    count = lax.axis_size(axis)
    leading, last = (max(0, -steps), min(count, count - steps))
    return lax.ppermute(value, axis, [(source, source + steps) for source in range(leading, last)])


def exchange(rows, experts):
    units = lax.axis_size("expert")
    cores = units // experts
    groups = [[e * cores + c for e in range(experts)] for c in range(cores)]
    parts = rows.reshape(experts, -1, rows.shape[1])
    swapped = lax.all_to_all(parts, "expert", 0, 0, axis_index_groups=groups, tiled=True)
    return swapped.reshape(rows.shape)


def on_device(
    section_inputs,
    stored_inputs,
    out_grads,
    fwd_routes,
    fwd_gates,
    fwd_modulation,
    bwd_routes,
    bwd_gates,
    bwd_modulation,
    up_weight,
    down_weight,
):
    units = lax.axis_size("expert")
    experts = units // 2
    tokens, width = section_inputs.shape[1:]
    cap = min(tokens, 5 * tokens // (2 * experts))
    slots = experts * cap
    ff = up_weight.shape[3]
    shape = jax.ShapeDtypeStruct
    sizes = dict(experts=experts, cap=cap)

    inputs, stored, grads = section_inputs[0], stored_inputs[0], out_grads[0]
    routes, gates = fwd_routes[0].T, fwd_gates[0].T
    routes_b, gates_b = bwd_routes[0].T, bwd_gates[0].T
    mod = fwd_modulation.reshape(3, 1, width)
    mod_b = bwd_modulation.reshape(3, 1, width)
    own = (up_weight[0, 0], down_weight[0, 0])
    swap = [(i, i ^ 1) for i in range(units)]
    other = tuple(lax.ppermute(w, "expert", swap) for w in own)

    (send,) = call(
        pack_fwd_body,
        [shape((SPLIT * slots, width // SPLIT), bf16)],
        (inputs, mod, routes),
        4 * tokens * slots * width,
        **sizes,
    )
    got = exchange(send, experts)

    send_b, normed_b, inv_b = call(
        pack_bwd_body,
        [
            shape((2 * SPLIT * slots, width // SPLIT), bf16),
            shape((tokens, width), f32),
            shape((tokens, 1), f32),
        ],
        (stored, grads, gates_b, mod_b, routes_b),
        12 * tokens * slots * width,
        **sizes,
    )
    got_b = exchange(send_b, experts)

    result = call_expert(expert_fwd_body, got, (own, other), 1, 8 * slots * width * ff, cap)
    back = exchange(result, experts)
    result_b = call_expert(expert_bwd_body, got_b, (own, other), 2, 12 * slots * width * ff, cap)
    back_b = exchange(result_b, experts)

    (out_fwd,) = call(
        combine_fwd_body,
        [shape((tokens, width), f32)],
        (back, gates, routes, inputs, mod),
        8 * tokens * slots * width,
        **sizes,
    )
    next_inputs = shifted(out_fwd[None], "section", 1)
    (section_grad,) = call(
        combine_bwd_body,
        [shape((tokens, width), bf16)],
        (back_b, routes_b, normed_b, inv_b, grads, mod_b),
        4 * tokens * slots * width,
        **sizes,
    )
    input_grads = shifted(section_grad[None], "section", -1)
    return (next_inputs, input_grads)


def solution(mesh):
    rows = P("section", "expert", None)
    mod = P("section", None, None)
    weight = P("section", "expert", None, None)
    placed = (rows, rows, rows, rows, rows, mod, rows, rows, mod, weight, weight)
    return jax.shard_map(
        on_device, mesh=mesh, in_specs=placed, out_specs=(rows, rows), check_vma=False
    )
```

```python
import functools

import jax
import jax.numpy as jnp
from jax import lax
from jax.experimental import pallas as pl
from jax.experimental.pallas import tpu as pltpu
from jax.sharding import PartitionSpec as P


norm_eps = 1e-06
f32 = jnp.float32
bf16 = jnp.bfloat16
SPLIT = 2
GROUP = 4
BLOCK = 512


def dot(a, b, dims=((1,), (0,))):
    return lax.dot_general(a, b, (dims, ((), ())), preferred_element_type=f32)


def iota(shape, dim):
    return lax.broadcasted_iota(jnp.int32, shape, dim)


def ones_where(cond):
    return jnp.where(cond, 1.0, 0.0)


def layer_norm(rows):
    mean_row = jnp.mean(rows, axis=-1, keepdims=True)
    centered = rows - mean_row
    variance = jnp.mean(centered * centered, axis=-1, keepdims=True)
    inv_std = lax.rsqrt(variance + norm_eps)
    return centered * inv_std, inv_std


def slots_of(routes, experts):
    tokens = routes.shape[1]
    earlier = ones_where(iota((tokens, tokens), 0) < iota((tokens, tokens), 1)).astype(bf16)
    numbers = iota((experts, tokens), 0)
    chosen = [ones_where(numbers == routes[k : k + 1, :]) for k in range(2)]
    before = [dot(c.astype(bf16), earlier) for c in chosen]
    before[1] = before[1] + jnp.sum(chosen[0], axis=1, keepdims=True)
    return [jnp.sum(b * c, axis=0, keepdims=True).astype(jnp.int32) for b, c in zip(before, chosen)]


def slot_rows(routes, experts, per_expert):
    slots = slots_of(routes, experts)
    return [routes[k : k + 1, :] * per_expert + slots[k] for k in range(2)]


def pack_fwd_body(x_ref, mod_ref, route_ref, out_ref, *, experts, cap):
    normed, _ = layer_norm(x_ref[...])
    hidden = (normed * (1.0 + mod_ref[1]) + mod_ref[0]).astype(bf16)
    part = hidden.shape[1] // SPLIT
    first = slot_rows(route_ref[...], experts, SPLIT * cap)
    numbers = iota((out_ref.shape[0], hidden.shape[0]), 0)
    left, right = [], []
    for h in range(SPLIT):
        hit = (numbers == first[0] + h * cap) | (numbers == first[1] + h * cap)
        left.append(ones_where(hit).astype(bf16))
        right.append(hidden[:, h * part : (h + 1) * part])
    out_ref[...] = dot(jnp.concatenate(left, 1), jnp.concatenate(right, 0)).astype(bf16)


def pack_bwd_body(place_ref, x_ref, g_ref, gate_ref, mod_ref, route_ref, *outs, experts, cap, side):
    blocks, norm_ref, inv_ref, where_ref = outs[:experts], *outs[experts:]
    normed, inv = layer_norm(x_ref[...])
    norm_ref[...] = normed
    inv_ref[...] = inv
    hidden = (normed * (1.0 + mod_ref[1]) + mod_ref[0]).astype(bf16)
    tokens, width = hidden.shape
    part = width // SPLIT
    scaled = mod_ref[2] * g_ref[...].astype(f32)
    routes = route_ref[...]
    slots = slots_of(routes, experts)
    back = [(routes[k : k + 1, :] * (SPLIT * cap) + slots[k]).astype(f32) for k in range(2)]
    columns = jnp.transpose(jnp.concatenate([gate_ref[...], *back] * 2, 0))
    where_ref[...] = columns.astype(jnp.int32)
    pair = [(columns[:, k : k + 1] * scaled).astype(bf16) for k in range(2)]
    shift = side.bit_length() - 1
    z, y = place_ref[0] >> shift, place_ref[0] & (side - 1)
    ahead = (((routes >> shift) - z) & (side - 1)) * side + ((routes - y) & (side - 1))
    first = [ahead[k : k + 1, :] * (2 * SPLIT * cap) + slots[k] for k in range(2)]
    numbers = iota((experts * 2 * SPLIT * cap, tokens), 0)
    left, right = [], []
    for h in range(SPLIT):
        hit = (numbers == first[0] + h * cap) | (numbers == first[1] + h * cap)
        left.append(ones_where(hit).astype(bf16))
        right.append(hidden[:, h * part : (h + 1) * part])
        for k in range(2):
            left.append(ones_where(numbers == first[k] + (SPLIT + h) * cap).astype(bf16))
            right.append(pair[k][:, h * part : (h + 1) * part])
    rows = dot(jnp.concatenate(left, 1), jnp.concatenate(right, 0)).astype(bf16)
    size = 2 * SPLIT * cap
    for n, block in enumerate(blocks):
        block[...] = rows[n * size : (n + 1) * size, :]


def regroup_matrix(kinds, cap, forward):
    size = GROUP * kinds * cap
    by_kind, by_source = iota((size, size), 0 if forward else 1), iota((size, size), 1 if forward else 0)

    def block_of(r):
        return jnp.floor((r.astype(f32) + 0.5) * (1.0 / cap)).astype(jnp.int32)

    kb, sb = block_of(by_kind), block_of(by_source)
    shift = kinds.bit_length() - 1
    same_slot = (by_kind - kb * cap) == (by_source - sb * cap)
    return ones_where(same_slot & (kb == (sb & (kinds - 1)) * GROUP + (sb >> shift))).astype(bf16)


def unpack(pieces, targets, cap):
    kinds = len(targets) * SPLIT
    matrix = regroup_matrix(kinds, cap, True)
    slab = GROUP * cap
    for n, piece in enumerate(pieces):
        rows = dot(matrix, piece).astype(bf16)
        part = rows.shape[1]
        for t, target in enumerate(targets):
            for h in range(SPLIT):
                kind = t * SPLIT + h
                target[n * slab : (n + 1) * slab, h * part : (h + 1) * part] = rows[kind * slab : (kind + 1) * slab, :]


def repack(sum_ref, cap):
    matrix = regroup_matrix(SPLIT, cap, False)
    slab, part = GROUP * cap, sum_ref.shape[1] // SPLIT
    for n in range(sum_ref.shape[0] // slab):
        rows = [sum_ref[n * slab : (n + 1) * slab, h * part : (h + 1) * part] for h in range(SPLIT)]
        yield n, dot(matrix, jnp.concatenate(rows, 0)).astype(bf16)


def fetches(pieces, sems):
    copies = [pltpu.make_async_copy(source, target, sems.at[n]) for n, (source, target) in enumerate(pieces)]
    for copy in copies:
        copy.start()
    return iter(copies)


def expert_fwd_body(x_ref, *refs, cap):
    weights, (out_ref, rows_ref, act_ref, sum_ref), buffers, sems = refs[:4], refs[4:8], refs[8:12], refs[12]
    size = GROUP * SPLIT * cap
    ff, width = weights[1].shape
    pieces = []
    for n in (0, 2):
        for j in range(0, ff, BLOCK):
            pieces.append((weights[n].at[:, j : j + BLOCK], buffers[n].at[:, j : j + BLOCK]))
    for j in range(0, width, BLOCK):
        for n in (1, 3):
            pieces.append((weights[n].at[:, j : j + BLOCK], buffers[n].at[:, j : j + BLOCK]))
    copies = fetches(pieces, sems)
    unpack([x_ref[n : n + size, :] for n in range(0, x_ref.shape[0], size)], [rows_ref], cap)
    for n, up in enumerate((buffers[0], buffers[2])):
        for j in range(0, ff, BLOCK):
            next(copies).wait()
            act = jax.nn.gelu(dot(rows_ref[...], up[:, j : j + BLOCK]))
            act_ref[:, n * ff + j : n * ff + j + BLOCK] = act.astype(bf16)
    for j in range(0, width, BLOCK):
        cols = slice(j, j + BLOCK)
        next(copies).wait()
        next(copies).wait()
        both = dot(act_ref[:, :ff], buffers[1][:, cols]) + dot(act_ref[:, ff:], buffers[3][:, cols])
        sum_ref[:, cols] = both.astype(bf16)
    for n, rows in repack(sum_ref, cap):
        out_ref[n * size : (n + 1) * size, :] = rows


def gelu_slope(x):
    c = 0.7978845608028654
    square = x * x
    t = jnp.tanh(c * x * (1.0 + 0.044715 * square))
    return 0.5 * (1.0 + t) + (0.5 * c) * x * (1.0 - t * t) * (1.0 + (3.0 * 0.044715) * square)


def expert_bwd_body(place_ref, *refs, cap, side):
    experts = side * side
    blocks, weights, refs = refs[:experts], refs[experts : experts + 4], refs[experts + 4 :]
    (out_ref, rows_ref, grads_ref, pre_ref, sum_ref), buffers, sems = refs[:5], refs[5:9], refs[9]
    ff, width = weights[1].shape
    transposed = ((1,), (1,))
    pieces = []
    for n in (0, 2):
        for j in range(0, ff, BLOCK):
            pieces.append((weights[n].at[:, j : j + BLOCK], buffers[n].at[:, j : j + BLOCK]))
            pieces.append((weights[n + 1].at[j : j + BLOCK, :], buffers[n + 1].at[j : j + BLOCK, :]))
    copies = fetches(pieces, sems)
    slabs = [jnp.concatenate([b[...] for b in blocks[n : n + GROUP]], 0) for n in range(0, experts, GROUP)]
    unpack(slabs, [rows_ref, grads_ref], cap)
    up_a, up_b = buffers[0], buffers[2]
    for n in range(2):
        up, down = buffers[2 * n], buffers[2 * n + 1]
        for j in range(0, ff, BLOCK):
            next(copies).wait()
            next(copies).wait()
            slope = gelu_slope(dot(rows_ref[...], up[:, j : j + BLOCK]))
            act_grad = dot(grads_ref[...], down[j : j + BLOCK, :], transposed)
            pre_ref[:, n * ff + j : n * ff + j + BLOCK] = (act_grad * slope).astype(bf16)
    for j in range(0, width, BLOCK):
        cols = slice(j, j + BLOCK)
        both = dot(pre_ref[:, :ff], up_a[cols, :], transposed) + dot(pre_ref[:, ff:], up_b[cols, :], transposed)
        sum_ref[:, cols] = both.astype(bf16)
    size = SPLIT * cap
    own_z, own_y = place_ref[0] >> (side.bit_length() - 1), place_ref[0] & (side - 1)
    for n, rows in repack(sum_ref, cap):
        for i in range(GROUP):
            behind = n * GROUP + i
            z, y = (own_z - behind // side) & (side - 1), (own_y - behind % side) & (side - 1)
            out_ref[z * side + y] = rows[i * size : (i + 1) * size, :]


def combine_fwd_body(r_ref, gate_ref, route_ref, x_ref, mod_ref, out_ref, *, experts, cap):
    tokens, width = x_ref.shape
    part = width // SPLIT
    first = slot_rows(route_ref[...], experts, SPLIT * cap)
    numbers = iota((r_ref.shape[0], tokens), 0)
    for h in range(SPLIT):
        weights = sum(jnp.where(numbers == first[k] + h * cap, gate_ref[k : k + 1, :], 0.0) for k in range(2))
        high = weights.astype(bf16)
        low = (weights - high.astype(f32)).astype(bf16)
        both = dot(high, r_ref[...], ((0,), (0,))) + dot(low, r_ref[...], ((0,), (0,)))
        cols = slice(h * part, (h + 1) * part)
        out_ref[:, cols] = x_ref[:, cols] + mod_ref[2][:, cols] * both


def combine_bwd_body(r_ref, where_ref, norm_far, inv_ref, g_far, mod_ref, out_ref, norm_ref, g_ref, sems, *, cap):
    copies = fetches([(norm_far, norm_ref), (g_far, g_ref)], sems)
    tokens = norm_ref.shape[0]
    numbers = iota((tokens, r_ref.shape[0]), 1)
    places = where_ref[...]
    halves = []
    for h in range(SPLIT):
        hit = (numbers == places[:, 2:3] + h * cap) | (numbers == places[:, 3:4] + h * cap)
        halves.append(dot(ones_where(hit).astype(bf16), r_ref[...]))
    dnorm = jnp.concatenate(halves, 1) * (1.0 + mod_ref[1])
    mean_one = jnp.mean(dnorm, axis=-1, keepdims=True)
    next(copies).wait()
    normed = norm_ref[...]
    mean_two = jnp.mean(dnorm * normed, axis=-1, keepdims=True)
    next(copies).wait()
    grad = g_ref[...].astype(f32) + (dnorm - mean_one - normed * mean_two) * inv_ref[...]
    out_ref[...] = grad.astype(bf16)


def in_hbm(*arrays):
    return [pltpu.with_memory_space_constraint(a, pltpu.HBM) for a in arrays]


def in_vmem(*arrays):
    return [pltpu.with_memory_space_constraint(a, pltpu.VMEM) for a in arrays]


def call(body, outs, args, flops, limit, scratch=(), scalars=0, far=(), **statics):
    return kernel(body, outs, args, flops, limit, scratch, scalars, far, **statics)


def kernel(body, outs, args, flops, limit, scratch, scalars, far, **statics):
    moved = sum(2 * a.size for a in args)
    specs = [pl.BlockSpec(memory_space=pltpu.SMEM) if n < scalars else pl.BlockSpec() for n in range(len(args))]
    for n in far:
        specs[n] = pl.BlockSpec(memory_space=pltpu.HBM)
    return pl.pallas_call(
        functools.partial(body, **statics),
        out_shape=outs,
        in_specs=specs,
        scratch_shapes=scratch,
        cost_estimate=pl.CostEstimate(flops=flops, bytes_accessed=moved, transcendentals=0),
        compiler_params=pltpu.CompilerParams(vmem_limit_bytes=limit << 20),
    )(*args)


def shifted(value, axis, steps):
    count = lax.axis_size(axis)
    leading, last = (max(0, -steps), min(count, count - steps))
    return lax.ppermute(value, axis, [(source, source + steps) for source in range(leading, last)])


def offset_by(block, number, side):
    units = lax.axis_size("expert")
    cores = units // (side * side)
    pairs = []
    for u in range(units):
        chip, core = u // cores, u % cores
        z, y = (chip // side + number // side) % side, (chip + number) % side
        pairs.append((u, (z * side + y) * cores + core))
    return lax.ppermute(block, "expert", pairs)


def exchange(rows, experts):
    units = lax.axis_size("expert")
    cores = units // experts
    groups = [[e * cores + c for e in range(experts)] for c in range(cores)]
    parts = rows.reshape(experts, -1, rows.shape[1])
    swapped = lax.all_to_all(parts, "expert", 0, 0, axis_index_groups=groups, tiled=True)
    return swapped.reshape(rows.shape)


def tick(
    section_inputs,
    stored_inputs,
    out_grads,
    fwd_routes,
    fwd_gates,
    fwd_modulation,
    bwd_routes,
    bwd_gates,
    bwd_modulation,
    up_weight,
    down_weight,
):
    units = lax.axis_size("expert")
    experts = units // 2
    tokens, width = section_inputs.shape[1:]
    cap = min(tokens, 5 * tokens // (2 * experts))
    slots = experts * cap
    ff = up_weight.shape[3]
    shape = jax.ShapeDtypeStruct
    sizes = dict(experts=experts, cap=cap)

    inputs, stored, grads = section_inputs[0], stored_inputs[0], out_grads[0]
    routes, gates = fwd_routes[0].T, fwd_gates[0].T
    routes_b, gates_b = bwd_routes[0].T, bwd_gates[0].T
    mod = fwd_modulation.reshape(3, 1, width)
    mod_b = bwd_modulation.reshape(3, 1, width)
    own = (up_weight[0, 0], down_weight[0, 0])
    swap = [(i, i ^ 1) for i in range(units)]
    weights = in_hbm(*own, *(lax.ppermute(w, "expert", swap) for w in own))
    side = 1 << (experts.bit_length() // 2)
    place = (lax.axis_index("expert") >> 1).astype(jnp.int32).reshape(1)
    half = width // SPLIT

    (send,) = call(
        pack_fwd_body,
        [shape((SPLIT * slots, half), bf16)],
        (inputs, mod, routes),
        4 * tokens * slots * width,
        60,
        **sizes,
    )
    got = exchange(send, experts)

    *blocks, normed_b, inv_b, where_b = call(
        pack_bwd_body,
        [pltpu.HBM((2 * SPLIT * cap, half), bf16)] * experts
        + [pltpu.HBM((tokens, width), f32), shape((tokens, 1), f32), shape((tokens, 8), jnp.int32)],
        (place, stored, grads, gates_b, mod_b, routes_b),
        12 * tokens * slots * width,
        28,
        scalars=1,
        side=side,
        **sizes,
    )
    got_b = in_hbm(blocks[0]) + [offset_by(b, n, side) for n, b in enumerate(blocks) if n > 0]

    rows_buffer = pltpu.VMEM((slots, width), bf16)
    hidden_buffer = pltpu.VMEM((slots, 2 * ff), bf16)
    weight_buffers = [pltpu.VMEM(w.shape, bf16) for w in weights] + [pltpu.SemaphoreType.DMA((16,))]
    (result,) = call(
        expert_fwd_body,
        [pltpu.HBM((SPLIT * slots, half), bf16)],
        (*in_vmem(got), *weights),
        8 * slots * width * ff,
        30,
        scratch=[rows_buffer, hidden_buffer, rows_buffer] + weight_buffers,
        far=(1, 2, 3, 4),
        cap=cap,
    )
    back = exchange(result, experts)
    (result_b,) = call(
        expert_bwd_body,
        [pltpu.HBM((experts, SPLIT * cap, half), bf16)],
        (place, *got_b, *weights),
        12 * slots * width * ff,
        36,
        scratch=[rows_buffer, rows_buffer, hidden_buffer, rows_buffer] + weight_buffers,
        far=range(experts + 1, experts + 5),
        scalars=1,
        cap=cap,
        side=side,
    )
    back_b = exchange(result_b.reshape(SPLIT * slots, half), experts)

    (out_fwd,) = call(
        combine_fwd_body,
        [pltpu.HBM((tokens, width), f32)],
        (*in_vmem(back), gates, routes, *in_hbm(inputs), mod),
        8 * tokens * slots * width,
        16,
        **sizes,
    )
    next_inputs = shifted(out_fwd[None], "section", 1)
    (section_grad,) = call(
        combine_bwd_body,
        [shape((tokens, width), bf16)],
        (*in_vmem(back_b), where_b, *in_hbm(normed_b), inv_b, *in_hbm(grads), mod_b),
        4 * tokens * slots * width,
        16,
        scratch=[pltpu.VMEM((tokens, width), f32), pltpu.VMEM((tokens, width), bf16), pltpu.SemaphoreType.DMA((2,))],
        far=(2, 4),
        cap=cap,
    )
    input_grads = shifted(section_grad[None], "section", -1)
    return (next_inputs, input_grads)


def solution(mesh):
    rows = P("section", "expert", None)
    mod = P("section", None, None)
    weight = P("section", "expert", None, None)
    placed = (rows, rows, rows, rows, rows, mod, rows, rows, mod, weight, weight)
    return jax.shard_map(tick, mesh=mesh, in_specs=placed, out_specs=(rows, rows), check_vma=False)
```

```python
import functools

import jax
import jax.numpy as jnp
from jax import lax
from jax.experimental import pallas as pl
from jax.experimental.pallas import tpu as pltpu
from jax.sharding import PartitionSpec as P


norm_eps = 1e-06
f32 = jnp.float32
bf16 = jnp.bfloat16
SPLIT = 2
GROUP = 4
BLOCK = 512
AHEAD = 12


def dot(a, b, dims=((1,), (0,))):
    return lax.dot_general(a, b, (dims, ((), ())), preferred_element_type=f32)


def iota(shape, dim):
    return lax.broadcasted_iota(jnp.int32, shape, dim)


def ones_where(cond):
    return jnp.where(cond, 1.0, 0.0)


def layer_norm(rows):
    mean_row = jnp.mean(rows, axis=-1, keepdims=True)
    centered = rows - mean_row
    variance = jnp.mean(centered * centered, axis=-1, keepdims=True)
    inv_std = lax.rsqrt(variance + norm_eps)
    return centered * inv_std, inv_std


def slots_of(routes, experts):
    tokens = routes.shape[1]
    earlier = ones_where(iota((tokens, tokens), 0) < iota((tokens, tokens), 1)).astype(bf16)
    numbers = iota((experts, tokens), 0)
    chosen = [ones_where(numbers == routes[k : k + 1, :]) for k in range(2)]
    before = [dot(c.astype(bf16), earlier) for c in chosen]
    before[1] = before[1] + jnp.sum(chosen[0], axis=1, keepdims=True)
    return [jnp.sum(b * c, axis=0, keepdims=True).astype(jnp.int32) for b, c in zip(before, chosen)]


def slot_rows(routes, experts, per_expert):
    slots = slots_of(routes, experts)
    return [routes[k : k + 1, :] * per_expert + slots[k] for k in range(2)]


def pack_fwd_body(x_ref, mod_ref, route_ref, out_ref, *, experts, cap):
    normed, _ = layer_norm(x_ref[...])
    hidden = (normed * (1.0 + mod_ref[1]) + mod_ref[0]).astype(bf16)
    part = hidden.shape[1] // SPLIT
    first = slot_rows(route_ref[...], experts, SPLIT * cap)
    numbers = iota((out_ref.shape[0], hidden.shape[0]), 0)
    left, right = [], []
    for h in range(SPLIT):
        hit = (numbers == first[0] + h * cap) | (numbers == first[1] + h * cap)
        left.append(ones_where(hit).astype(bf16))
        right.append(hidden[:, h * part : (h + 1) * part])
    out_ref[...] = dot(jnp.concatenate(left, 1), jnp.concatenate(right, 0)).astype(bf16)


def pack_bwd_body(place_ref, x_ref, g_ref, gate_ref, mod_ref, route_ref, *outs, experts, cap, side):
    blocks, (norm_far, inv_ref, where_ref, norm_ref, right_ref, out_ref, sems) = outs[:experts], outs[experts:]
    normed, inv = layer_norm(x_ref[...])
    norm_ref[...] = normed
    copies = sends([(norm_ref, norm_far)], sems, 0)
    inv_ref[...] = inv
    hidden = (normed * (1.0 + mod_ref[1]) + mod_ref[0]).astype(bf16)
    tokens, width = hidden.shape
    part = width // SPLIT
    scaled = mod_ref[2] * g_ref[...].astype(f32)
    routes = route_ref[...]
    slots = slots_of(routes, experts)
    back = [(routes[k : k + 1, :] * (SPLIT * cap) + slots[k]).astype(f32) for k in range(2)]
    columns = jnp.transpose(jnp.concatenate([gate_ref[...], *back] * 2, 0))
    where_ref[...] = columns.astype(jnp.int32)
    shift = side.bit_length() - 1
    z, y = place_ref[0] >> shift, place_ref[0] & (side - 1)
    ahead = (((routes >> shift) - z) & (side - 1)) * side + ((routes - y) & (side - 1))
    first = [ahead[k : k + 1, :] * (2 * SPLIT * cap) + slots[k] for k in range(2)]
    for n, value in enumerate((hidden, *((columns[:, k : k + 1] * scaled).astype(bf16) for k in range(2)))):
        for h in range(SPLIT):
            at = (3 * h + n) * tokens
            right_ref[at : at + tokens, :] = value[:, h * part : (h + 1) * part]
    size = 2 * SPLIT * cap
    for n in range(0, experts, GROUP):
        numbers = iota((GROUP * size, tokens), 0) + n * size
        left = []
        for h in range(SPLIT):
            hit = (numbers == first[0] + h * cap) | (numbers == first[1] + h * cap)
            left.append(ones_where(hit).astype(bf16))
            for k in range(2):
                left.append(ones_where(numbers == first[k] + (SPLIT + h) * cap).astype(bf16))
        out_ref[n * size : (n + GROUP) * size, :] = dot(jnp.concatenate(left, 1), right_ref[...]).astype(bf16)
        pieces = [(out_ref.at[m * size : (m + 1) * size, :], blocks[m]) for m in range(n, n + GROUP)]
        copies += sends(pieces, sems, len(copies))
    for copy in copies:
        copy.wait()


def regroup_matrix(kinds, cap, forward):
    size = GROUP * kinds * cap
    by_kind, by_source = iota((size, size), 0 if forward else 1), iota((size, size), 1 if forward else 0)

    def block_of(r):
        return jnp.floor((r.astype(f32) + 0.5) * (1.0 / cap)).astype(jnp.int32)

    kb, sb = block_of(by_kind), block_of(by_source)
    shift = kinds.bit_length() - 1
    same_slot = (by_kind - kb * cap) == (by_source - sb * cap)
    return ones_where(same_slot & (kb == (sb & (kinds - 1)) * GROUP + (sb >> shift))).astype(bf16)


def unpack(pieces, targets, cap):
    kinds = len(targets) * SPLIT
    matrix = regroup_matrix(kinds, cap, True)
    slab = GROUP * cap
    for n, piece in enumerate(pieces):
        rows = dot(matrix, piece).astype(bf16)
        part = rows.shape[1]
        for t, target in enumerate(targets):
            for h in range(SPLIT):
                kind = t * SPLIT + h
                target[n * slab : (n + 1) * slab, h * part : (h + 1) * part] = rows[kind * slab : (kind + 1) * slab, :]


def repack(halves, cap):
    matrix = regroup_matrix(SPLIT, cap, False)
    slab = GROUP * cap
    for n in range(halves[0].shape[0] // slab):
        yield n, dot(matrix, jnp.concatenate([v[n * slab : (n + 1) * slab, :] for v in halves], 0)).astype(bf16)


def fetches(pieces, sems, ahead):
    copies = [pltpu.make_async_copy(source, target, sems.at[n]) for n, (source, target) in enumerate(pieces)]
    for copy in copies[:ahead]:
        copy.start()
    for n, copy in enumerate(copies):
        copy.wait()
        for later in copies[n + ahead : n + ahead + 1]:
            later.start()
        yield


def sends(pieces, sems, first):
    copies = [pltpu.make_async_copy(s, t, sems.at[first + n]) for n, (s, t) in enumerate(pieces)]
    for copy in copies:
        copy.start()
    return copies


def expert_fwd_body(x_ref, *refs, cap):
    weights, (out_far, rows_ref, act_ref, out_ref), buffers, sems = refs[:4], refs[4:8], refs[8:12], refs[12]
    size = GROUP * SPLIT * cap
    ff, width = weights[1].shape
    part = width // SPLIT
    columns = [h * part + j for j in range(0, part, BLOCK) for h in range(SPLIT)]
    pieces = []
    for n in (0, 2):
        for j in range(0, ff, BLOCK):
            pieces.append((weights[n].at[:, j : j + BLOCK], buffers[n].at[:, j : j + BLOCK]))
    for j in columns:
        for n in (1, 3):
            pieces.append((weights[n].at[:, j : j + BLOCK], buffers[n].at[:, j : j + BLOCK]))
    ready = fetches(pieces, sems, AHEAD)
    unpack([x_ref[n : n + size, :] for n in range(0, x_ref.shape[0], size)], [rows_ref], cap)
    for n, up in enumerate((buffers[0], buffers[2])):
        for j in range(0, ff, BLOCK):
            next(ready)
            act = jax.nn.gelu(dot(rows_ref[...], up[:, j : j + BLOCK]))
            act_ref[:, n * ff + j : n * ff + j + BLOCK] = act.astype(bf16)
    halves, copies = [], []
    for j in columns:
        cols = slice(j, j + BLOCK)
        next(ready)
        next(ready)
        both = dot(act_ref[:, :ff], buffers[1][:, cols]) + dot(act_ref[:, ff:], buffers[3][:, cols])
        halves.append(both.astype(bf16))
        if len(halves) == SPLIT:
            cols = slice(j % part, j % part + BLOCK)
            for n, rows in repack(halves, cap):
                out_ref[n * size : (n + 1) * size, cols] = rows
            copies += sends([(out_ref.at[:, cols], out_far.at[:, cols])], sems, len(pieces) + len(copies))
            halves = []
    for copy in copies:
        copy.wait()


def gelu_slope(x):
    c = 0.7978845608028654
    square = x * x
    t = jnp.tanh(c * x * (1.0 + 0.044715 * square))
    return 0.5 * (1.0 + t) + (0.5 * c) * x * (1.0 - t * t) * (1.0 + (3.0 * 0.044715) * square)


def expert_bwd_body(place_ref, *refs, cap, side):
    experts = side * side
    blocks, weights, refs = refs[:experts], refs[experts : experts + 4], refs[experts + 4 :]
    (out_far, rows_ref, grads_ref, pre_ref, out_ref), buffers, sems = refs[:5], refs[5:9], refs[9]
    ff, width = weights[1].shape
    part = width // SPLIT
    transposed = ((1,), (1,))
    pieces = []
    for n in (0, 2):
        for j in range(0, ff, BLOCK):
            pieces.append((weights[n].at[:, j : j + BLOCK], buffers[n].at[:, j : j + BLOCK]))
            pieces.append((weights[n + 1].at[j : j + BLOCK, :], buffers[n + 1].at[j : j + BLOCK, :]))
    ready = fetches(pieces, sems, AHEAD)
    slabs = [jnp.concatenate([b[...] for b in blocks[n : n + GROUP]], 0) for n in range(0, experts, GROUP)]
    unpack(slabs, [rows_ref, grads_ref], cap)
    up_a, up_b = buffers[0], buffers[2]
    for n in range(2):
        up, down = buffers[2 * n], buffers[2 * n + 1]
        for j in range(0, ff, BLOCK):
            next(ready)
            next(ready)
            slope = gelu_slope(dot(rows_ref[...], up[:, j : j + BLOCK]))
            act_grad = dot(grads_ref[...], down[j : j + BLOCK, :], transposed)
            pre_ref[:, n * ff + j : n * ff + j + BLOCK] = (act_grad * slope).astype(bf16)
    size = SPLIT * cap
    own_z, own_y = place_ref[0] >> (side.bit_length() - 1), place_ref[0] & (side - 1)
    copies = []
    for j in range(0, part, BLOCK):
        halves = []
        for h in range(SPLIT):
            cols = slice(h * part + j, h * part + j + BLOCK)
            both = dot(pre_ref[:, :ff], up_a[cols, :], transposed) + dot(pre_ref[:, ff:], up_b[cols, :], transposed)
            halves.append(both.astype(bf16))
        cols = slice(j, j + BLOCK)
        for n, rows in repack(halves, cap):
            for i in range(GROUP):
                behind = n * GROUP + i
                z, y = (own_z - behind // side) & (side - 1), (own_y - behind % side) & (side - 1)
                out_ref[z * side + y, :, cols] = rows[i * size : (i + 1) * size, :]
        copies += sends([(out_ref.at[:, :, cols], out_far.at[:, :, cols])], sems, len(pieces) + len(copies))
    for copy in copies:
        copy.wait()


def settle_body(x_ref, out_ref):
    out_ref[...] = x_ref[...]


def combine_fwd_body(r_ref, gate_ref, route_ref, x_ref, mod_ref, out_ref, *, experts, cap):
    tokens, width = x_ref.shape
    part = width // SPLIT
    first = slot_rows(route_ref[...], experts, SPLIT * cap)
    numbers = iota((r_ref.shape[0], tokens), 0)
    for h in range(SPLIT):
        weights = sum(jnp.where(numbers == first[k] + h * cap, gate_ref[k : k + 1, :], 0.0) for k in range(2))
        high = weights.astype(bf16)
        low = (weights - high.astype(f32)).astype(bf16)
        both = dot(high, r_ref[...], ((0,), (0,))) + dot(low, r_ref[...], ((0,), (0,)))
        cols = slice(h * part, (h + 1) * part)
        out_ref[:, cols] = x_ref[:, cols] + mod_ref[2][:, cols] * both


def combine_bwd_body(r_ref, where_ref, norm_far, inv_ref, g_far, mod_ref, out_ref, norm_ref, g_ref, sems, *, cap):
    ready = fetches([(norm_far, norm_ref), (g_far, g_ref)], sems, 2)
    tokens = norm_ref.shape[0]
    numbers = iota((tokens, r_ref.shape[0]), 1)
    places = where_ref[...]
    halves = []
    for h in range(SPLIT):
        hit = (numbers == places[:, 2:3] + h * cap) | (numbers == places[:, 3:4] + h * cap)
        halves.append(dot(ones_where(hit).astype(bf16), r_ref[...]))
    dnorm = jnp.concatenate(halves, 1) * (1.0 + mod_ref[1])
    mean_one = jnp.mean(dnorm, axis=-1, keepdims=True)
    next(ready)
    normed = norm_ref[...]
    mean_two = jnp.mean(dnorm * normed, axis=-1, keepdims=True)
    next(ready)
    grad = g_ref[...].astype(f32) + (dnorm - mean_one - normed * mean_two) * inv_ref[...]
    out_ref[...] = grad.astype(bf16)


def in_hbm(*arrays):
    return [pltpu.with_memory_space_constraint(a, pltpu.HBM) for a in arrays]


def in_vmem(*arrays):
    return [pltpu.with_memory_space_constraint(a, pltpu.VMEM) for a in arrays]


def call(body, outs, args, flops, limit, scratch=(), scalars=0, far=(), far_outs=(), **statics):
    return kernel(body, outs, args, flops, limit, scratch, scalars, far, far_outs, **statics)


def kernel(body, outs, args, flops, limit, scratch, scalars, far, far_outs, **statics):
    moved = sum(2 * a.size for a in args)
    specs = [pl.BlockSpec(memory_space=pltpu.SMEM) if n < scalars else pl.BlockSpec() for n in range(len(args))]
    for n in far:
        specs[n] = pl.BlockSpec(memory_space=pltpu.HBM)
    return pl.pallas_call(
        functools.partial(body, **statics),
        out_shape=outs,
        in_specs=specs,
        out_specs=[pl.BlockSpec(memory_space=pltpu.HBM) if n in far_outs else pl.BlockSpec() for n in range(len(outs))],
        scratch_shapes=scratch,
        cost_estimate=pl.CostEstimate(flops=flops, bytes_accessed=moved, transcendentals=0),
        compiler_params=pltpu.CompilerParams(vmem_limit_bytes=limit << 20),
    )(*args)


def shifted(value, axis, steps):
    count = lax.axis_size(axis)
    leading, last = (max(0, -steps), min(count, count - steps))
    return lax.ppermute(value, axis, [(source, source + steps) for source in range(leading, last)])


def offset_by(block, number, side):
    units = lax.axis_size("expert")
    cores = units // (side * side)
    pairs = []
    for u in range(units):
        chip, core = u // cores, u % cores
        z, y = (chip // side + number // side) % side, (chip + number) % side
        pairs.append((u, (z * side + y) * cores + core))
    return lax.ppermute(block, "expert", pairs)


def exchange(rows, experts):
    units = lax.axis_size("expert")
    cores = units // experts
    groups = [[e * cores + c for e in range(experts)] for c in range(cores)]
    parts = rows.reshape(experts, -1, rows.shape[1])
    swapped = lax.all_to_all(parts, "expert", 0, 0, axis_index_groups=groups, tiled=True)
    return swapped.reshape(rows.shape)


def tick(
    section_inputs,
    stored_inputs,
    out_grads,
    fwd_routes,
    fwd_gates,
    fwd_modulation,
    bwd_routes,
    bwd_gates,
    bwd_modulation,
    up_weight,
    down_weight,
):
    units = lax.axis_size("expert")
    experts = units // 2
    tokens, width = section_inputs.shape[1:]
    cap = min(tokens, 5 * tokens // (2 * experts))
    slots = experts * cap
    ff = up_weight.shape[3]
    shape = jax.ShapeDtypeStruct
    sizes = dict(experts=experts, cap=cap)

    inputs, stored, grads = section_inputs[0], stored_inputs[0], out_grads[0]
    routes, gates = fwd_routes[0].T, fwd_gates[0].T
    routes_b, gates_b = bwd_routes[0].T, bwd_gates[0].T
    mod = fwd_modulation.reshape(3, 1, width)
    mod_b = bwd_modulation.reshape(3, 1, width)
    own = (up_weight[0, 0], down_weight[0, 0])
    swap = [(i, i ^ 1) for i in range(units)]
    weights = in_hbm(*own, *(lax.ppermute(w, "expert", swap) for w in own))
    side = 1 << (experts.bit_length() // 2)
    place = (lax.axis_index("expert") >> 1).astype(jnp.int32).reshape(1)
    half = width // SPLIT

    (send,) = call(
        pack_fwd_body,
        [pltpu.HBM((SPLIT * slots, half), bf16)],
        (*in_hbm(inputs), mod, routes),
        4 * tokens * slots * width,
        60,
        **sizes,
    )
    got = exchange(send, experts)

    *blocks, normed_b, inv_b, where_b = call(
        pack_bwd_body,
        [pltpu.HBM((2 * SPLIT * cap, half), bf16)] * experts
        + [pltpu.HBM((tokens, width), f32), shape((tokens, 1), f32), shape((tokens, 8), jnp.int32)],
        (place, stored, grads, gates_b, mod_b, routes_b),
        12 * tokens * slots * width,
        28,
        scratch=[
            pltpu.VMEM((tokens, width), f32),
            pltpu.VMEM((3 * SPLIT * tokens, half), bf16),
            pltpu.VMEM((2 * SPLIT * slots, half), bf16),
            pltpu.SemaphoreType.DMA((experts + 1,)),
        ],
        scalars=1,
        far_outs=range(experts + 1),
        side=side,
        **sizes,
    )
    got_b = in_hbm(blocks[0]) + [offset_by(b, n, side) for n, b in enumerate(blocks) if n > 0]

    rows_buffer = pltpu.VMEM((slots, width), bf16)
    hidden_buffer = pltpu.VMEM((slots, 2 * ff), bf16)
    weight_buffers = [pltpu.VMEM(w.shape, bf16) for w in weights] + [pltpu.SemaphoreType.DMA((20,))]
    (result,) = call(
        expert_fwd_body,
        [pltpu.HBM((SPLIT * slots, half), bf16)],
        (*in_vmem(got), *weights),
        8 * slots * width * ff,
        30,
        scratch=[rows_buffer, hidden_buffer, pltpu.VMEM((SPLIT * slots, half), bf16)] + weight_buffers,
        far=(1, 2, 3, 4),
        far_outs=(0,),
        cap=cap,
    )
    back = exchange(result, experts)
    (result_b,) = call(
        expert_bwd_body,
        [pltpu.HBM((experts, SPLIT * cap, half), bf16)],
        (place, *got_b, *weights),
        12 * slots * width * ff,
        36,
        scratch=[rows_buffer, rows_buffer, hidden_buffer, pltpu.VMEM((experts, SPLIT * cap, half), bf16)]
        + weight_buffers,
        far=range(experts + 1, experts + 5),
        far_outs=(0,),
        scalars=1,
        cap=cap,
        side=side,
    )
    back_b = exchange(result_b.reshape(SPLIT * slots, half), experts)

    (out_fwd,) = call(
        combine_fwd_body,
        [pltpu.HBM((tokens, width), f32)],
        (*in_vmem(back), gates, routes, *in_hbm(inputs), mod),
        8 * tokens * slots * width,
        16,
        **sizes,
    )
    next_inputs = shifted(out_fwd[None], "section", 1)
    (section_grad,) = call(
        combine_bwd_body,
        [shape((tokens, width), bf16)],
        (*in_vmem(back_b), where_b, *in_hbm(normed_b), inv_b, *in_hbm(grads), mod_b),
        4 * tokens * slots * width,
        16,
        scratch=[pltpu.VMEM((tokens, width), f32), pltpu.VMEM((tokens, width), bf16), pltpu.SemaphoreType.DMA((2,))],
        far=(2, 4),
        cap=cap,
    )
    input_grads = shifted(section_grad[None], "section", -1)
    (next_inputs,) = call(settle_body, [shape((tokens, width), f32)], (next_inputs[0],), 1000, 8)
    next_inputs = next_inputs[None]
    return (next_inputs, input_grads)


def solution(mesh):
    rows = P("section", "expert", None)
    mod = P("section", None, None)
    weight = P("section", "expert", None, None)
    placed = (rows, rows, rows, rows, rows, mod, rows, rows, mod, weight, weight)
    return jax.shard_map(tick, mesh=mesh, in_specs=placed, out_specs=(rows, rows), check_vma=False)
```

```python
import functools

import jax
import jax.numpy as jnp
from jax import lax
from jax.experimental import pallas as pl
from jax.experimental.pallas import tpu as pltpu
from jax.sharding import PartitionSpec as P


norm_eps = 1e-06
f32 = jnp.float32
bf16 = jnp.bfloat16
SPLIT = 2
GROUP = 4
BLOCK = 512
AHEAD = 12


def dot(a, b, dims=((1,), (0,))):
    return lax.dot_general(a, b, (dims, ((), ())), preferred_element_type=f32)


def iota(shape, dim):
    return lax.broadcasted_iota(jnp.int32, shape, dim)


def ones_where(cond):
    return jnp.where(cond, 1.0, 0.0)


def layer_norm(rows):
    mean_row = jnp.mean(rows, axis=-1, keepdims=True)
    centered = rows - mean_row
    variance = jnp.mean(centered * centered, axis=-1, keepdims=True)
    inv_std = lax.rsqrt(variance + norm_eps)
    return centered * inv_std, inv_std


def slots_of(routes, experts):
    tokens = routes.shape[1]
    earlier = ones_where(iota((tokens, tokens), 0) < iota((tokens, tokens), 1)).astype(bf16)
    numbers = iota((experts, tokens), 0)
    chosen = [ones_where(numbers == routes[k : k + 1, :]) for k in range(2)]
    before = [dot(c.astype(bf16), earlier) for c in chosen]
    before[1] = before[1] + jnp.sum(chosen[0], axis=1, keepdims=True)
    return [jnp.sum(b * c, axis=0, keepdims=True).astype(jnp.int32) for b, c in zip(before, chosen)]


def slot_rows(routes, experts, per_expert):
    slots = slots_of(routes, experts)
    return [routes[k : k + 1, :] * per_expert + slots[k] for k in range(2)]


def pack_fwd_body(x_ref, mod_ref, route_ref, out_ref, *, experts, cap):
    normed, _ = layer_norm(x_ref[...])
    hidden = (normed * (1.0 + mod_ref[1]) + mod_ref[0]).astype(bf16)
    part = hidden.shape[1] // SPLIT
    first = slot_rows(route_ref[...], experts, SPLIT * cap)
    numbers = iota((out_ref.shape[0], hidden.shape[0]), 0)
    left, right = [], []
    for h in range(SPLIT):
        hit = (numbers == first[0] + h * cap) | (numbers == first[1] + h * cap)
        left.append(ones_where(hit).astype(bf16))
        right.append(hidden[:, h * part : (h + 1) * part])
    out_ref[...] = dot(jnp.concatenate(left, 1), jnp.concatenate(right, 0)).astype(bf16)


def pack_bwd_body(place_ref, x_ref, g_ref, gate_ref, mod_ref, route_ref, *outs, experts, cap):
    blocks, (norm_far, inv_ref, where_ref, norm_ref, right_ref, out_ref, sems) = outs[:experts], outs[experts:]
    normed, inv = layer_norm(x_ref[...])
    norm_ref[...] = normed
    copies = sends([(norm_ref, norm_far)], sems, 0)
    inv_ref[...] = inv
    hidden = (normed * (1.0 + mod_ref[1]) + mod_ref[0]).astype(bf16)
    tokens, width = hidden.shape
    part = width // SPLIT
    scaled = mod_ref[2] * g_ref[...].astype(f32)
    routes = route_ref[...]
    slots = slots_of(routes, experts)
    back = [(routes[k : k + 1, :] * (SPLIT * cap) + slots[k]).astype(f32) for k in range(2)]
    columns = jnp.transpose(jnp.concatenate([gate_ref[...], *back] * 2, 0))
    where_ref[...] = columns.astype(jnp.int32)
    ahead = routes ^ place_ref[0]
    first = [ahead[k : k + 1, :] * (2 * SPLIT * cap) + slots[k] for k in range(2)]
    for n, value in enumerate((hidden, *((columns[:, k : k + 1] * scaled).astype(bf16) for k in range(2)))):
        for h in range(SPLIT):
            at = (3 * h + n) * tokens
            right_ref[at : at + tokens, :] = value[:, h * part : (h + 1) * part]
    size = 2 * SPLIT * cap
    for n in range(0, experts, GROUP):
        numbers = iota((GROUP * size, tokens), 0) + n * size
        left = []
        for h in range(SPLIT):
            hit = (numbers == first[0] + h * cap) | (numbers == first[1] + h * cap)
            left.append(ones_where(hit).astype(bf16))
            for k in range(2):
                left.append(ones_where(numbers == first[k] + (SPLIT + h) * cap).astype(bf16))
        out_ref[n * size : (n + GROUP) * size, :] = dot(jnp.concatenate(left, 1), right_ref[...]).astype(bf16)
        pieces = [(out_ref.at[m * size : (m + 1) * size, :], blocks[m]) for m in range(n, n + GROUP)]
        copies += sends(pieces, sems, len(copies))
    for copy in copies:
        copy.wait()


def regroup_matrix(kinds, cap, forward):
    size = GROUP * kinds * cap
    by_kind, by_source = iota((size, size), 0 if forward else 1), iota((size, size), 1 if forward else 0)

    def block_of(r):
        return jnp.floor((r.astype(f32) + 0.5) * (1.0 / cap)).astype(jnp.int32)

    kb, sb = block_of(by_kind), block_of(by_source)
    shift = kinds.bit_length() - 1
    same_slot = (by_kind - kb * cap) == (by_source - sb * cap)
    return ones_where(same_slot & (kb == (sb & (kinds - 1)) * GROUP + (sb >> shift))).astype(bf16)


def unpack(pieces, targets, cap):
    kinds = len(targets) * SPLIT
    matrix = regroup_matrix(kinds, cap, True)
    slab = GROUP * cap
    for n, piece in enumerate(pieces):
        rows = dot(matrix, piece).astype(bf16)
        part = rows.shape[1]
        for t, target in enumerate(targets):
            for h in range(SPLIT):
                kind = t * SPLIT + h
                target[n * slab : (n + 1) * slab, h * part : (h + 1) * part] = rows[kind * slab : (kind + 1) * slab, :]


def repack(halves, cap):
    matrix = regroup_matrix(SPLIT, cap, False)
    slab = GROUP * cap
    for n in range(halves[0].shape[0] // slab):
        yield n, dot(matrix, jnp.concatenate([v[n * slab : (n + 1) * slab, :] for v in halves], 0)).astype(bf16)


def fetches(pieces, sems, ahead):
    copies = [pltpu.make_async_copy(source, target, sems.at[n]) for n, (source, target) in enumerate(pieces)]
    for copy in copies[:ahead]:
        copy.start()
    for n, copy in enumerate(copies):
        copy.wait()
        for later in copies[n + ahead : n + ahead + 1]:
            later.start()
        yield


def sends(pieces, sems, first):
    copies = [pltpu.make_async_copy(s, t, sems.at[first + n]) for n, (s, t) in enumerate(pieces)]
    for copy in copies:
        copy.start()
    return copies


def expert_fwd_body(x_ref, *refs, cap):
    weights, (out_far, rows_ref, act_ref, out_ref), buffers, sems = refs[:4], refs[4:8], refs[8:12], refs[12]
    size = GROUP * SPLIT * cap
    ff, width = weights[1].shape
    part = width // SPLIT
    columns = [h * part + j for j in range(0, part, BLOCK) for h in range(SPLIT)]
    pieces = []
    for n in (0, 2):
        for j in range(0, ff, BLOCK):
            pieces.append((weights[n].at[:, j : j + BLOCK], buffers[n].at[:, j : j + BLOCK]))
    for j in columns:
        for n in (1, 3):
            pieces.append((weights[n].at[:, j : j + BLOCK], buffers[n].at[:, j : j + BLOCK]))
    ready = fetches(pieces, sems, AHEAD)
    unpack([x_ref[n : n + size, :] for n in range(0, x_ref.shape[0], size)], [rows_ref], cap)
    for n, up in enumerate((buffers[0], buffers[2])):
        for j in range(0, ff, BLOCK):
            next(ready)
            act = jax.nn.gelu(dot(rows_ref[...], up[:, j : j + BLOCK]))
            act_ref[:, n * ff + j : n * ff + j + BLOCK] = act.astype(bf16)
    halves, copies = [], []
    for j in columns:
        cols = slice(j, j + BLOCK)
        next(ready)
        next(ready)
        both = dot(act_ref[:, :ff], buffers[1][:, cols]) + dot(act_ref[:, ff:], buffers[3][:, cols])
        halves.append(both.astype(bf16))
        if len(halves) == SPLIT:
            cols = slice(j % part, j % part + BLOCK)
            for n, rows in repack(halves, cap):
                out_ref[n * size : (n + 1) * size, cols] = rows
            copies += sends([(out_ref.at[:, cols], out_far.at[:, cols])], sems, len(pieces) + len(copies))
            halves = []
    for copy in copies:
        copy.wait()


def gelu_slope(x):
    c = 0.7978845608028654
    square = x * x
    t = jnp.tanh(c * x * (1.0 + 0.044715 * square))
    return 0.5 * (1.0 + t) + (0.5 * c) * x * (1.0 - t * t) * (1.0 + (3.0 * 0.044715) * square)


def expert_bwd_body(place_ref, *refs, cap):
    experts = len(refs) - 14
    blocks, weights, refs = refs[:experts], refs[experts : experts + 4], refs[experts + 4 :]
    (out_far, rows_ref, grads_ref, pre_ref, out_ref), buffers, sems = refs[:5], refs[5:9], refs[9]
    ff, width = weights[1].shape
    part = width // SPLIT
    transposed = ((1,), (1,))
    pieces = []
    for n in (0, 2):
        for j in range(0, ff, BLOCK):
            pieces.append((weights[n].at[:, j : j + BLOCK], buffers[n].at[:, j : j + BLOCK]))
            pieces.append((weights[n + 1].at[j : j + BLOCK, :], buffers[n + 1].at[j : j + BLOCK, :]))
    ready = fetches(pieces, sems, AHEAD)
    slabs = [jnp.concatenate([b[...] for b in blocks[n : n + GROUP]], 0) for n in range(0, experts, GROUP)]
    unpack(slabs, [rows_ref, grads_ref], cap)
    up_a, up_b = buffers[0], buffers[2]
    for n in range(2):
        up, down = buffers[2 * n], buffers[2 * n + 1]
        for j in range(0, ff, BLOCK):
            next(ready)
            next(ready)
            slope = gelu_slope(dot(rows_ref[...], up[:, j : j + BLOCK]))
            act_grad = dot(grads_ref[...], down[j : j + BLOCK, :], transposed)
            pre_ref[:, n * ff + j : n * ff + j + BLOCK] = (act_grad * slope).astype(bf16)
    size = SPLIT * cap
    copies = []
    for j in range(0, part, BLOCK):
        halves = []
        for h in range(SPLIT):
            cols = slice(h * part + j, h * part + j + BLOCK)
            both = dot(pre_ref[:, :ff], up_a[cols, :], transposed) + dot(pre_ref[:, ff:], up_b[cols, :], transposed)
            halves.append(both.astype(bf16))
        cols = slice(j, j + BLOCK)
        for n, rows in repack(halves, cap):
            for i in range(GROUP):
                out_ref[place_ref[0] ^ (n * GROUP + i), :, cols] = rows[i * size : (i + 1) * size, :]
        copies += sends([(out_ref.at[:, :, cols], out_far.at[:, :, cols])], sems, len(pieces) + len(copies))
    for copy in copies:
        copy.wait()


def settle_body(x_ref, out_ref):
    out_ref[...] = x_ref[...]


def combine_fwd_body(r_ref, gate_ref, route_ref, x_ref, mod_ref, out_ref, *, experts, cap):
    tokens, width = x_ref.shape
    part = width // SPLIT
    first = slot_rows(route_ref[...], experts, SPLIT * cap)
    numbers = iota((r_ref.shape[0], tokens), 0)
    for h in range(SPLIT):
        weights = sum(jnp.where(numbers == first[k] + h * cap, gate_ref[k : k + 1, :], 0.0) for k in range(2))
        high = weights.astype(bf16)
        low = (weights - high.astype(f32)).astype(bf16)
        both = dot(high, r_ref[...], ((0,), (0,))) + dot(low, r_ref[...], ((0,), (0,)))
        cols = slice(h * part, (h + 1) * part)
        out_ref[:, cols] = x_ref[:, cols] + mod_ref[2][:, cols] * both


def combine_bwd_body(r_ref, where_ref, norm_far, inv_ref, g_far, mod_ref, out_ref, norm_ref, g_ref, sems, *, cap):
    ready = fetches([(norm_far, norm_ref), (g_far, g_ref)], sems, 2)
    tokens = norm_ref.shape[0]
    numbers = iota((tokens, r_ref.shape[0]), 1)
    places = where_ref[...]
    halves = []
    for h in range(SPLIT):
        hit = (numbers == places[:, 2:3] + h * cap) | (numbers == places[:, 3:4] + h * cap)
        halves.append(dot(ones_where(hit).astype(bf16), r_ref[...]))
    dnorm = jnp.concatenate(halves, 1) * (1.0 + mod_ref[1])
    mean_one = jnp.mean(dnorm, axis=-1, keepdims=True)
    next(ready)
    normed = norm_ref[...]
    mean_two = jnp.mean(dnorm * normed, axis=-1, keepdims=True)
    next(ready)
    grad = g_ref[...].astype(f32) + (dnorm - mean_one - normed * mean_two) * inv_ref[...]
    out_ref[...] = grad.astype(bf16)


def in_hbm(*arrays):
    return [pltpu.with_memory_space_constraint(a, pltpu.HBM) for a in arrays]


def in_vmem(*arrays):
    return [pltpu.with_memory_space_constraint(a, pltpu.VMEM) for a in arrays]


def call(body, outs, args, flops, limit, scratch=(), scalars=0, far=(), far_outs=(), **statics):
    return kernel(body, outs, args, flops, limit, scratch, scalars, far, far_outs, **statics)


def kernel(body, outs, args, flops, limit, scratch, scalars, far, far_outs, **statics):
    moved = sum(2 * a.size for a in args)
    specs = [pl.BlockSpec(memory_space=pltpu.SMEM) if n < scalars else pl.BlockSpec() for n in range(len(args))]
    for n in far:
        specs[n] = pl.BlockSpec(memory_space=pltpu.HBM)
    return pl.pallas_call(
        functools.partial(body, **statics),
        out_shape=outs,
        in_specs=specs,
        out_specs=[pl.BlockSpec(memory_space=pltpu.HBM) if n in far_outs else pl.BlockSpec() for n in range(len(outs))],
        scratch_shapes=scratch,
        cost_estimate=pl.CostEstimate(flops=flops, bytes_accessed=moved, transcendentals=0),
        compiler_params=pltpu.CompilerParams(vmem_limit_bytes=limit << 20),
    )(*args)


def shifted(value, axis, steps):
    count = lax.axis_size(axis)
    leading, last = (max(0, -steps), min(count, count - steps))
    return lax.ppermute(value, axis, [(source, source + steps) for source in range(leading, last)])


def trade(block, number):
    pairs = [(u, (u // 2 ^ number) * 2 + u % 2) for u in range(lax.axis_size("expert"))]
    return lax.ppermute(block, "expert", pairs)


def exchange(rows, experts):
    units = lax.axis_size("expert")
    cores = units // experts
    groups = [[e * cores + c for e in range(experts)] for c in range(cores)]
    parts = rows.reshape(experts, -1, rows.shape[1])
    swapped = lax.all_to_all(parts, "expert", 0, 0, axis_index_groups=groups, tiled=True)
    return swapped.reshape(rows.shape)


def tick(
    section_inputs,
    stored_inputs,
    out_grads,
    fwd_routes,
    fwd_gates,
    fwd_modulation,
    bwd_routes,
    bwd_gates,
    bwd_modulation,
    up_weight,
    down_weight,
):
    units = lax.axis_size("expert")
    experts = units // 2
    tokens, width = section_inputs.shape[1:]
    cap = min(tokens, 5 * tokens // (2 * experts))
    slots = experts * cap
    ff = up_weight.shape[3]
    shape = jax.ShapeDtypeStruct
    sizes = dict(experts=experts, cap=cap)

    inputs, stored, grads = section_inputs[0], stored_inputs[0], out_grads[0]
    routes, gates = fwd_routes[0].T, fwd_gates[0].T
    routes_b, gates_b = bwd_routes[0].T, bwd_gates[0].T
    mod = fwd_modulation.reshape(3, 1, width)
    mod_b = bwd_modulation.reshape(3, 1, width)
    own = (up_weight[0, 0], down_weight[0, 0])
    swap = [(i, i ^ 1) for i in range(units)]
    weights = in_hbm(*own, *(lax.ppermute(w, "expert", swap) for w in own))
    place = (lax.axis_index("expert") >> 1).astype(jnp.int32).reshape(1)
    half = width // SPLIT

    (send,) = call(
        pack_fwd_body,
        [pltpu.HBM((SPLIT * slots, half), bf16)],
        (*in_hbm(inputs), mod, routes),
        4 * tokens * slots * width,
        60,
        **sizes,
    )
    got = exchange(send, experts)

    *blocks, normed_b, inv_b, where_b = call(
        pack_bwd_body,
        [pltpu.HBM((2 * SPLIT * cap, half), bf16)] * experts
        + [pltpu.HBM((tokens, width), f32), shape((tokens, 1), f32), shape((tokens, 8), jnp.int32)],
        (place, stored, grads, gates_b, mod_b, routes_b),
        12 * tokens * slots * width,
        28,
        scratch=[
            pltpu.VMEM((tokens, width), f32),
            pltpu.VMEM((3 * SPLIT * tokens, half), bf16),
            pltpu.VMEM((2 * SPLIT * slots, half), bf16),
            pltpu.SemaphoreType.DMA((experts + 1,)),
        ],
        scalars=1,
        far_outs=range(experts + 1),
        **sizes,
    )
    got_b = in_hbm(blocks[0]) + [trade(b, n) for n, b in enumerate(blocks) if n > 0]

    rows_buffer = pltpu.VMEM((slots, width), bf16)
    hidden_buffer = pltpu.VMEM((slots, 2 * ff), bf16)
    weight_buffers = [pltpu.VMEM(w.shape, bf16) for w in weights] + [pltpu.SemaphoreType.DMA((20,))]
    (result,) = call(
        expert_fwd_body,
        [pltpu.HBM((SPLIT * slots, half), bf16)],
        (*in_vmem(got), *weights),
        8 * slots * width * ff,
        30,
        scratch=[rows_buffer, hidden_buffer, pltpu.VMEM((SPLIT * slots, half), bf16)] + weight_buffers,
        far=(1, 2, 3, 4),
        far_outs=(0,),
        cap=cap,
    )
    back = exchange(result, experts)
    (result_b,) = call(
        expert_bwd_body,
        [pltpu.HBM((experts, SPLIT * cap, half), bf16)],
        (place, *got_b, *weights),
        12 * slots * width * ff,
        36,
        scratch=[rows_buffer, rows_buffer, hidden_buffer, pltpu.VMEM((experts, SPLIT * cap, half), bf16)]
        + weight_buffers,
        far=range(experts + 1, experts + 5),
        far_outs=(0,),
        scalars=1,
        cap=cap,
    )
    back_b = exchange(result_b.reshape(SPLIT * slots, half), experts)

    (out_fwd,) = call(
        combine_fwd_body,
        [pltpu.HBM((tokens, width), f32)],
        (*in_vmem(back), gates, routes, *in_hbm(inputs), mod),
        8 * tokens * slots * width,
        16,
        **sizes,
    )
    next_inputs = shifted(out_fwd[None], "section", 1)
    (section_grad,) = call(
        combine_bwd_body,
        [shape((tokens, width), bf16)],
        (*in_vmem(back_b), where_b, *in_hbm(normed_b), inv_b, *in_hbm(grads), mod_b),
        4 * tokens * slots * width,
        16,
        scratch=[pltpu.VMEM((tokens, width), f32), pltpu.VMEM((tokens, width), bf16), pltpu.SemaphoreType.DMA((2,))],
        far=(2, 4),
        cap=cap,
    )
    input_grads = shifted(section_grad[None], "section", -1)
    (next_inputs,) = call(settle_body, [shape((tokens, width), f32)], (next_inputs[0],), 1000, 8)
    next_inputs = next_inputs[None]
    return (next_inputs, input_grads)


def solution(mesh):
    rows = P("section", "expert", None)
    mod = P("section", None, None)
    weight = P("section", "expert", None, None)
    placed = (rows, rows, rows, rows, rows, mod, rows, rows, mod, weight, weight)
    return jax.shard_map(tick, mesh=mesh, in_specs=placed, out_specs=(rows, rows), check_vma=False)
```

```python
import functools

import jax
import jax.numpy as jnp
from jax import lax
from jax.experimental import pallas as pl
from jax.experimental.pallas import tpu as pltpu
from jax.sharding import PartitionSpec as P


norm_eps = 1e-06
f32 = jnp.float32
bf16 = jnp.bfloat16
SPLIT = 2
GROUP = 4
BLOCK = 512
AHEAD = 12


def dot(a, b, dims=((1,), (0,))):
    return lax.dot_general(a, b, (dims, ((), ())), preferred_element_type=f32)


def iota(shape, dim):
    return lax.broadcasted_iota(jnp.int32, shape, dim)


def ones_where(cond):
    return jnp.where(cond, 1.0, 0.0)


def layer_norm(rows):
    mean_row = jnp.mean(rows, axis=-1, keepdims=True)
    centered = rows - mean_row
    variance = jnp.mean(centered * centered, axis=-1, keepdims=True)
    inv_std = lax.rsqrt(variance + norm_eps)
    return centered * inv_std, inv_std


def slots_of(routes, experts):
    tokens = routes.shape[1]
    earlier = ones_where(iota((tokens, tokens), 0) < iota((tokens, tokens), 1)).astype(bf16)
    numbers = iota((experts, tokens), 0)
    chosen = [ones_where(numbers == routes[k : k + 1, :]) for k in range(2)]
    before = [dot(c.astype(bf16), earlier) for c in chosen]
    before[1] = before[1] + jnp.sum(chosen[0], axis=1, keepdims=True)
    return [jnp.sum(b * c, axis=0, keepdims=True).astype(jnp.int32) for b, c in zip(before, chosen)]


def slot_rows(routes, experts, per_expert):
    slots = slots_of(routes, experts)
    return [routes[k : k + 1, :] * per_expert + slots[k] for k in range(2)]


def pack_fwd_body(x_ref, mod_ref, route_ref, out_ref, *, experts, cap):
    normed, _ = layer_norm(x_ref[...])
    hidden = (normed * (1.0 + mod_ref[1]) + mod_ref[0]).astype(bf16)
    part = hidden.shape[1] // SPLIT
    first = slot_rows(route_ref[...], experts, SPLIT * cap)
    numbers = iota((out_ref.shape[0], hidden.shape[0]), 0)
    left, right = [], []
    for h in range(SPLIT):
        hit = (numbers == first[0] + h * cap) | (numbers == first[1] + h * cap)
        left.append(ones_where(hit).astype(bf16))
        right.append(hidden[:, h * part : (h + 1) * part])
    out_ref[...] = dot(jnp.concatenate(left, 1), jnp.concatenate(right, 0)).astype(bf16)


def pack_bwd_body(place_ref, x_ref, g_ref, gate_ref, mod_ref, route_ref, *outs, experts, cap):
    blocks, (norm_far, inv_ref, where_ref, norm_ref, right_ref, out_ref, sems) = outs[:experts], outs[experts:]
    normed, inv = layer_norm(x_ref[...])
    norm_ref[...] = normed
    copies = sends([(norm_ref, norm_far)], sems, 0)
    inv_ref[...] = inv
    hidden = (normed * (1.0 + mod_ref[1]) + mod_ref[0]).astype(bf16)
    tokens, width = hidden.shape
    part = width // SPLIT
    scaled = mod_ref[2] * g_ref[...].astype(f32)
    routes = route_ref[...]
    slots = slots_of(routes, experts)
    back = [(routes[k : k + 1, :] * (SPLIT * cap) + slots[k]).astype(f32) for k in range(2)]
    columns = jnp.transpose(jnp.concatenate([gate_ref[...], *back] * 2, 0))
    where_ref[...] = columns.astype(jnp.int32)
    ahead = routes ^ place_ref[0]
    first = [ahead[k : k + 1, :] * (2 * SPLIT * cap) + slots[k] for k in range(2)]
    for n, value in enumerate((hidden, *((columns[:, k : k + 1] * scaled).astype(bf16) for k in range(2)))):
        for h in range(SPLIT):
            at = (3 * h + n) * tokens
            right_ref[at : at + tokens, :] = value[:, h * part : (h + 1) * part]
    size = 2 * SPLIT * cap
    for n in range(0, experts, GROUP):
        numbers = iota((GROUP * size, tokens), 0) + n * size
        left = []
        for h in range(SPLIT):
            hit = (numbers == first[0] + h * cap) | (numbers == first[1] + h * cap)
            left.append(ones_where(hit).astype(bf16))
            for k in range(2):
                left.append(ones_where(numbers == first[k] + (SPLIT + h) * cap).astype(bf16))
        out_ref[n * size : (n + GROUP) * size, :] = dot(jnp.concatenate(left, 1), right_ref[...]).astype(bf16)
        pieces = [(out_ref.at[m * size : (m + 1) * size, :], blocks[m]) for m in range(n, n + GROUP)]
        copies += sends(pieces, sems, len(copies))
    for copy in copies:
        copy.wait()


def regroup_matrix(kinds, cap, forward):
    size = GROUP * kinds * cap
    by_kind, by_source = iota((size, size), 0 if forward else 1), iota((size, size), 1 if forward else 0)

    def block_of(r):
        return jnp.floor((r.astype(f32) + 0.5) * (1.0 / cap)).astype(jnp.int32)

    kb, sb = block_of(by_kind), block_of(by_source)
    shift = kinds.bit_length() - 1
    same_slot = (by_kind - kb * cap) == (by_source - sb * cap)
    return ones_where(same_slot & (kb == (sb & (kinds - 1)) * GROUP + (sb >> shift))).astype(bf16)


def unpack(pieces, targets, cap):
    kinds = len(targets) * SPLIT
    matrix = regroup_matrix(kinds, cap, True)
    slab = GROUP * cap
    for n, piece in enumerate(pieces):
        rows = dot(matrix, piece).astype(bf16)
        part = rows.shape[1]
        for t, target in enumerate(targets):
            for h in range(SPLIT):
                kind = t * SPLIT + h
                target[n * slab : (n + 1) * slab, h * part : (h + 1) * part] = rows[kind * slab : (kind + 1) * slab, :]


def repack(halves, cap):
    matrix = regroup_matrix(SPLIT, cap, False)
    slab = GROUP * cap
    for n in range(halves[0].shape[0] // slab):
        yield n, dot(matrix, jnp.concatenate([v[n * slab : (n + 1) * slab, :] for v in halves], 0)).astype(bf16)


def fetches(pieces, sems, ahead):
    copies = [pltpu.make_async_copy(source, target, sems.at[n]) for n, (source, target) in enumerate(pieces)]
    for copy in copies[:ahead]:
        copy.start()
    for n, copy in enumerate(copies):
        copy.wait()
        for later in copies[n + ahead : n + ahead + 1]:
            later.start()
        yield


def sends(pieces, sems, first):
    copies = [pltpu.make_async_copy(s, t, sems.at[first + n]) for n, (s, t) in enumerate(pieces)]
    for copy in copies:
        copy.start()
    return copies


def expert_fwd_body(x_ref, *refs, cap):
    weights, (out_far, rows_ref, act_ref, out_ref), buffers, sems = refs[:4], refs[4:8], refs[8:12], refs[12]
    size = GROUP * SPLIT * cap
    ff, width = weights[1].shape
    part = width // SPLIT
    columns = [h * part + j for j in range(0, part, BLOCK) for h in range(SPLIT)]
    pieces = []
    for n in (0, 2):
        for j in range(0, ff, BLOCK):
            pieces.append((weights[n].at[:, j : j + BLOCK], buffers[n].at[:, j : j + BLOCK]))
    for j in columns:
        for n in (1, 3):
            pieces.append((weights[n].at[:, j : j + BLOCK], buffers[n].at[:, j : j + BLOCK]))
    ready = fetches(pieces, sems, AHEAD)
    unpack([x_ref[n : n + size, :] for n in range(0, x_ref.shape[0], size)], [rows_ref], cap)
    for n, up in enumerate((buffers[0], buffers[2])):
        for j in range(0, ff, BLOCK):
            next(ready)
            act = jax.nn.gelu(dot(rows_ref[...], up[:, j : j + BLOCK]))
            act_ref[:, n * ff + j : n * ff + j + BLOCK] = act.astype(bf16)
    halves, copies = [], []
    for j in columns:
        cols = slice(j, j + BLOCK)
        next(ready)
        next(ready)
        both = dot(act_ref[:, :ff], buffers[1][:, cols]) + dot(act_ref[:, ff:], buffers[3][:, cols])
        halves.append(both.astype(bf16))
        if len(halves) == SPLIT:
            cols = slice(j % part, j % part + BLOCK)
            for n, rows in repack(halves, cap):
                out_ref[n * size : (n + 1) * size, cols] = rows
            copies += sends([(out_ref.at[:, cols], out_far.at[:, cols])], sems, len(pieces) + len(copies))
            halves = []
    for copy in copies:
        copy.wait()


def gelu_slope(x):
    c = 0.7978845608028654
    square = x * x
    t = jnp.tanh(c * x * (1.0 + 0.044715 * square))
    return 0.5 * (1.0 + t) + (0.5 * c) * x * (1.0 - t * t) * (1.0 + (3.0 * 0.044715) * square)


def expert_bwd_body(place_ref, *refs, cap):
    experts = len(refs) - 14
    blocks, weights, refs = refs[:experts], refs[experts : experts + 4], refs[experts + 4 :]
    (out_far, rows_ref, grads_ref, pre_ref, out_ref), buffers, sems = refs[:5], refs[5:9], refs[9]
    ff, width = weights[1].shape
    part = width // SPLIT
    transposed = ((1,), (1,))
    pieces = []
    for n in (0, 2):
        for j in range(0, ff, BLOCK):
            pieces.append((weights[n].at[:, j : j + BLOCK], buffers[n].at[:, j : j + BLOCK]))
            pieces.append((weights[n + 1].at[j : j + BLOCK, :], buffers[n + 1].at[j : j + BLOCK, :]))
    ready = fetches(pieces, sems, AHEAD)
    slabs = [jnp.concatenate([b[...] for b in blocks[n : n + GROUP]], 0) for n in range(0, experts, GROUP)]
    unpack(slabs, [rows_ref, grads_ref], cap)
    up_a, up_b = buffers[0], buffers[2]
    for n in range(2):
        up, down = buffers[2 * n], buffers[2 * n + 1]
        for j in range(0, ff, BLOCK):
            next(ready)
            next(ready)
            slope = gelu_slope(dot(rows_ref[...], up[:, j : j + BLOCK]))
            act_grad = dot(grads_ref[...], down[j : j + BLOCK, :], transposed)
            pre_ref[:, n * ff + j : n * ff + j + BLOCK] = (act_grad * slope).astype(bf16)
    size = SPLIT * cap
    copies = []
    for j in range(0, part, BLOCK):
        halves = []
        for h in range(SPLIT):
            cols = slice(h * part + j, h * part + j + BLOCK)
            both = dot(pre_ref[:, :ff], up_a[cols, :], transposed) + dot(pre_ref[:, ff:], up_b[cols, :], transposed)
            halves.append(both.astype(bf16))
        cols = slice(j, j + BLOCK)
        for n, rows in repack(halves, cap):
            for i in range(GROUP):
                out_ref[place_ref[0] ^ (n * GROUP + i), :, cols] = rows[i * size : (i + 1) * size, :]
        copies += sends([(out_ref.at[:, :, cols], out_far.at[:, :, cols])], sems, len(pieces) + len(copies))
    for copy in copies:
        copy.wait()


def settle_body(x_ref, out_ref):
    out_ref[...] = x_ref[...]


def combine_fwd_body(r_ref, gate_ref, route_ref, x_ref, mod_ref, out_ref, *, experts, cap):
    tokens, width = x_ref.shape
    part = width // SPLIT
    first = slot_rows(route_ref[...], experts, SPLIT * cap)
    numbers = iota((r_ref.shape[0], tokens), 0)
    for h in range(SPLIT):
        weights = sum(jnp.where(numbers == first[k] + h * cap, gate_ref[k : k + 1, :], 0.0) for k in range(2))
        high = weights.astype(bf16)
        low = (weights - high.astype(f32)).astype(bf16)
        both = dot(high, r_ref[...], ((0,), (0,))) + dot(low, r_ref[...], ((0,), (0,)))
        cols = slice(h * part, (h + 1) * part)
        out_ref[:, cols] = x_ref[:, cols] + mod_ref[2][:, cols] * both


def combine_bwd_body(r_ref, where_ref, norm_far, inv_ref, g_far, mod_ref, out_ref, norm_ref, g_ref, sems, *, cap):
    ready = fetches([(norm_far, norm_ref), (g_far, g_ref)], sems, 2)
    tokens = norm_ref.shape[0]
    numbers = iota((tokens, r_ref.shape[0]), 1)
    places = where_ref[...]
    picks = []
    for h in range(SPLIT):
        hit = (numbers == places[:, 2:3] + h * cap) | (numbers == places[:, 3:4] + h * cap)
        picks.append(ones_where(hit).astype(bf16))
    both = dot(jnp.concatenate(picks, 0), r_ref[...])
    halves = [both[h * tokens : (h + 1) * tokens, :] for h in range(SPLIT)]
    dnorm = jnp.concatenate(halves, 1) * (1.0 + mod_ref[1])
    mean_one = jnp.mean(dnorm, axis=-1, keepdims=True)
    next(ready)
    normed = norm_ref[...]
    mean_two = jnp.mean(dnorm * normed, axis=-1, keepdims=True)
    next(ready)
    grad = g_ref[...].astype(f32) + (dnorm - mean_one - normed * mean_two) * inv_ref[...]
    out_ref[...] = grad.astype(bf16)


def in_hbm(*arrays):
    return [pltpu.with_memory_space_constraint(a, pltpu.HBM) for a in arrays]


def in_vmem(*arrays):
    return [pltpu.with_memory_space_constraint(a, pltpu.VMEM) for a in arrays]


def call(body, outs, args, flops, limit, scratch=(), scalars=0, far=(), far_outs=(), **statics):
    return kernel(body, outs, args, flops, limit, scratch, scalars, far, far_outs, **statics)


def kernel(body, outs, args, flops, limit, scratch, scalars, far, far_outs, **statics):
    moved = sum(2 * a.size for a in args)
    specs = [pl.BlockSpec(memory_space=pltpu.SMEM) if n < scalars else pl.BlockSpec() for n in range(len(args))]
    for n in far:
        specs[n] = pl.BlockSpec(memory_space=pltpu.HBM)
    return pl.pallas_call(
        functools.partial(body, **statics),
        out_shape=outs,
        in_specs=specs,
        out_specs=[pl.BlockSpec(memory_space=pltpu.HBM) if n in far_outs else pl.BlockSpec() for n in range(len(outs))],
        scratch_shapes=scratch,
        cost_estimate=pl.CostEstimate(flops=flops, bytes_accessed=moved, transcendentals=0),
        compiler_params=pltpu.CompilerParams(vmem_limit_bytes=limit << 20),
    )(*args)


def shifted(value, axis, steps):
    count = lax.axis_size(axis)
    leading, last = (max(0, -steps), min(count, count - steps))
    return lax.ppermute(value, axis, [(source, source + steps) for source in range(leading, last)])


def trade(block, number):
    pairs = [(u, (u // 2 ^ number) * 2 + u % 2) for u in range(lax.axis_size("expert"))]
    return lax.ppermute(block, "expert", pairs)


def exchange(rows, experts):
    units = lax.axis_size("expert")
    cores = units // experts
    groups = [[e * cores + c for e in range(experts)] for c in range(cores)]
    parts = rows.reshape(experts, -1, rows.shape[1])
    swapped = lax.all_to_all(parts, "expert", 0, 0, axis_index_groups=groups, tiled=True)
    return swapped.reshape(rows.shape)


def tick(
    section_inputs,
    stored_inputs,
    out_grads,
    fwd_routes,
    fwd_gates,
    fwd_modulation,
    bwd_routes,
    bwd_gates,
    bwd_modulation,
    up_weight,
    down_weight,
):
    units = lax.axis_size("expert")
    experts = units // 2
    tokens, width = section_inputs.shape[1:]
    cap = min(tokens, 5 * tokens // (2 * experts))
    slots = experts * cap
    ff = up_weight.shape[3]
    shape = jax.ShapeDtypeStruct
    sizes = dict(experts=experts, cap=cap)

    inputs, stored, grads = section_inputs[0], stored_inputs[0], out_grads[0]
    routes, gates = fwd_routes[0].T, fwd_gates[0].T
    routes_b, gates_b = bwd_routes[0].T, bwd_gates[0].T
    mod = fwd_modulation.reshape(3, 1, width)
    mod_b = bwd_modulation.reshape(3, 1, width)
    own = (up_weight[0, 0], down_weight[0, 0])
    swap = [(i, i ^ 1) for i in range(units)]
    weights = in_hbm(*own, *(lax.ppermute(w, "expert", swap) for w in own))
    place = (lax.axis_index("expert") >> 1).astype(jnp.int32).reshape(1)
    half = width // SPLIT

    (send,) = call(
        pack_fwd_body,
        [pltpu.HBM((SPLIT * slots, half), bf16)],
        (*in_hbm(inputs), mod, routes),
        4 * tokens * slots * width,
        60,
        **sizes,
    )
    got = exchange(send, experts)

    *blocks, normed_b, inv_b, where_b = call(
        pack_bwd_body,
        [pltpu.HBM((2 * SPLIT * cap, half), bf16)] * experts
        + [pltpu.HBM((tokens, width), f32), shape((tokens, 1), f32), shape((tokens, 8), jnp.int32)],
        (place, stored, grads, gates_b, mod_b, routes_b),
        12 * tokens * slots * width,
        28,
        scratch=[
            pltpu.VMEM((tokens, width), f32),
            pltpu.VMEM((3 * SPLIT * tokens, half), bf16),
            pltpu.VMEM((2 * SPLIT * slots, half), bf16),
            pltpu.SemaphoreType.DMA((experts + 1,)),
        ],
        scalars=1,
        far_outs=range(experts + 1),
        **sizes,
    )
    got_b = in_hbm(blocks[0]) + [trade(b, n) for n, b in enumerate(blocks) if n > 0]

    rows_buffer = pltpu.VMEM((slots, width), bf16)
    hidden_buffer = pltpu.VMEM((slots, 2 * ff), bf16)
    weight_buffers = [pltpu.VMEM(w.shape, bf16) for w in weights] + [pltpu.SemaphoreType.DMA((20,))]
    (result,) = call(
        expert_fwd_body,
        [pltpu.HBM((SPLIT * slots, half), bf16)],
        (*in_vmem(got), *weights),
        8 * slots * width * ff,
        30,
        scratch=[rows_buffer, hidden_buffer, pltpu.VMEM((SPLIT * slots, half), bf16)] + weight_buffers,
        far=(1, 2, 3, 4),
        far_outs=(0,),
        cap=cap,
    )
    back = exchange(result, experts)
    (result_b,) = call(
        expert_bwd_body,
        [pltpu.HBM((experts, SPLIT * cap, half), bf16)],
        (place, *got_b, *weights),
        12 * slots * width * ff,
        36,
        scratch=[rows_buffer, rows_buffer, hidden_buffer, pltpu.VMEM((experts, SPLIT * cap, half), bf16)]
        + weight_buffers,
        far=range(experts + 1, experts + 5),
        far_outs=(0,),
        scalars=1,
        cap=cap,
    )
    back_b = exchange(result_b.reshape(SPLIT * slots, half), experts)

    (out_fwd,) = call(
        combine_fwd_body,
        [pltpu.HBM((tokens, width), f32)],
        (*in_vmem(back), gates, routes, *in_hbm(inputs), mod),
        8 * tokens * slots * width,
        16,
        **sizes,
    )
    next_inputs = shifted(out_fwd[None], "section", 1)
    (section_grad,) = call(
        combine_bwd_body,
        [shape((tokens, width), bf16)],
        (*in_vmem(back_b), where_b, *in_hbm(normed_b), inv_b, *in_hbm(grads), mod_b),
        4 * tokens * slots * width,
        16,
        scratch=[pltpu.VMEM((tokens, width), f32), pltpu.VMEM((tokens, width), bf16), pltpu.SemaphoreType.DMA((2,))],
        far=(2, 4),
        cap=cap,
    )
    input_grads = shifted(section_grad[None], "section", -1)
    (next_inputs,) = call(settle_body, [shape((tokens, width), f32)], (next_inputs[0],), 1000, 8)
    next_inputs = next_inputs[None]
    return (next_inputs, input_grads)


def solution(mesh):
    rows = P("section", "expert", None)
    mod = P("section", None, None)
    weight = P("section", "expert", None, None)
    placed = (rows, rows, rows, rows, rows, mod, rows, rows, mod, weight, weight)
    return jax.shard_map(tick, mesh=mesh, in_specs=placed, out_specs=(rows, rows), check_vma=False)
```
